256 devices in a mesh: trial: 4 (over z_lo), ep: 4 (over y), fsdp: 16 (over z_hi, x, core).
Axes of the slice: x: 4, y: 4, z: 8 (z_hi: 2, z_lo: 4; z = z_hi * 4 + z_lo), core: 2. Of those that a mesh axis runs over, the one named last changes fastest.
Arguments:
- master_down: float32 [256, 1024, 2048], P(('trial', 'ep'), None, 'fsdp'), parts along dimension 0, may hold values from -0.25 to 0.25
- router_weight: float32 [8192, 64], P(('trial', 'fsdp'), 'ep'), parts along dimension 0, may hold values from -0.125 to 0.125
- router_gain: float32 [8192], P(('trial', 'fsdp')), parts along dimension 0, may hold values from 0.25 to 1.75
Outputs:
- final_down: bfloat16 [256, 1024, 2048], P(('trial', 'ep'), 'fsdp'), parts along dimension 0
- scale_down: float32 [256, 1024], P(('trial', 'ep'), 'fsdp'), parts along dimension 0
- serve_router: bfloat16 [8192, 64], P('trial'), parts along dimension 0
The draws below stay inside these ranges and needn't reach their ends.
There are 4 independent parts, one for each index of `trial`. The reference program is written for one: setup_inputs(seed, part) draws one part's arguments, and reference() takes and returns one part's arrays. A program takes and returns all parts, laid end to end along the dimension named above; each array names one. Nothing has to cross between parts.
All inputs are finite; a program needn't handle non-finite values. Where the reference program divides by a largest or mean magnitude, that divisor is 1e-20 or more.
Results may differ from the reference program's by a relative error of at most 0.001.
Values may be sent and summed in bfloat16 or wider, within the bound.
No kernel may reach another device: no remote copies, remote signals or barrier semaphores. Data moves between devices by JAX's collectives and lax.ppermute only.
A program may use at most 64 MiB of HBM per device.

```python
import jax
import jax.numpy as jnp

EXPERTS = 64
D_MODEL = 2048
D_EXPERT = 1024


def strengthened(array, key, source, target, shards_of, factor):
    def block_of(position):
        return (jnp.arange(array.shape[position]) // (array.shape[position] // shards_of)).reshape((-1,) + (1,) * (array.ndim - 1 - position))

    first = jax.random.permutation(key, shards_of)[block_of(target)]
    second = (block_of(target) + shards_of // 2) % shards_of
    return jnp.where((block_of(source) == first) | (block_of(source) == second), factor * array, array)


def block_scale(own_key, dims, cuts, smallest, largest):
    level = 1.0
    for axis_at, shards_of in cuts:
        draws = jax.random.uniform(jax.random.fold_in(jax.random.fold_in(own_key, 6), axis_at), (shards_of,), jnp.float32, smallest / len(cuts), largest / len(cuts))
        level = level * jnp.repeat(jnp.exp(draws), dims[axis_at] // shards_of).reshape((-1,) + (1,) * (len(dims) - 1 - axis_at))
    return level


def centred(own_key, shape, scale, bound, pieces=(), kind=jnp.bfloat16):
    result = jax.random.normal(own_key, shape, jnp.float32) * scale
    if len(pieces) > 0:
        result = block_scale(own_key, shape, pieces, -0.22, 0.18) * result
    return jnp.clip(result, min=-bound, max=bound).astype(kind)


def bell_draw_with(rng, extent, deviation, reach, split, heavy, kind=jnp.bfloat16):
    result = deviation * jax.random.normal(rng, extent, jnp.float32)
    if split:
        result = result * block_scale(rng, extent, split, -0.22, 0.18)
    return jnp.clip(strengthened(result, jax.random.fold_in(rng, 3), *heavy), -reach, reach).astype(kind)


def setup_inputs(seed: int = 0, part: int = 0) -> dict:
    arg_keys = jax.random.split(jax.random.key(seed), 4)
    part_splits = jax.random.split(jax.random.fold_in(arg_keys[3], part), 4)
    master_down = bell_draw_with(part_splits[0], (EXPERTS, D_EXPERT, D_MODEL), D_EXPERT ** -0.5, 0.25, ((0, 4), (2, 16)), (2, 1, 16, 2.0), jnp.float32)
    router_weight = centred(part_splits[1], (D_MODEL, EXPERTS), D_MODEL ** -0.5, 0.125, ((0, 16), (1, 4)), jnp.float32)
    router_gain = jnp.clip(1.0 + 0.15 * jax.random.normal(part_splits[2], (D_MODEL,), jnp.float32), 0.25, 1.75)
    return dict(master_down=master_down, router_weight=router_weight, router_gain=router_gain)


def reference(master_down, router_weight, router_gain):
    scale_down = jnp.max(jnp.abs(master_down), axis=2)
    final_down = (master_down / jnp.expand_dims(scale_down, 2)).astype(jnp.bfloat16)
    serve_router = (router_weight * router_gain[:, None]).astype(jnp.bfloat16)
    return final_down, scale_down, serve_router
```

```python
import functools

import jax
import jax.numpy as jnp
from jax import lax
from jax.experimental import pallas as pl
from jax.experimental.pallas import tpu as pltpu
from jax.sharding import PartitionSpec as P


EARLY = 1
BF16, F32 = jnp.bfloat16, jnp.float32
ANY = pl.BlockSpec(memory_space=pl.ANY)
VMEM = pl.BlockSpec(memory_space=pltpu.VMEM)
SMEM = pl.BlockSpec(memory_space=pltpu.SMEM)
HOPS = [(dx, dc) for dx in range(4) for dc in range(2)]


def params(mebibytes):
    return pltpu.CompilerParams(vmem_limit_bytes=mebibytes * 2**20)


def cost(read, written):
    return pl.CostEstimate(flops=(read + written) * 4, bytes_accessed=read + written, transcendentals=0)


def route(dz, dx, dc):
    pairs = []
    for f in range(16):
        z, x, c = f // 8, f // 2 % 4, f % 2
        pairs.append((f, (z ^ dz) * 8 + (x + dx) % 4 * 2 + (c ^ dc)))
    return pairs


def partner(f, dz, dx, dc):
    z, x, c = f // 8, f // 2 % 4, f % 2
    z = z if dz == 0 else 1 - z
    c = c if dc == 0 else 1 - c
    return z * 8 + (x + dx) % 4 * 2 + c


def lanes(position):
    return pl.ds(pl.multiple_of(position * 128, 128), 128)


def local_kernel(w_ref, router_ref, gain_ref, out_ref, taken, sems):
    blocks, experts = taken.shape[:2]
    reads = []
    for b in range(blocks):
        reads.append(pltpu.make_async_copy(w_ref.at[:, pl.ds(128 * b, 128), :], taken.at[b], sems.at[b]))
        reads[-1].start()
    out_ref[:, 128 * blocks :] = router_ref[...] * gain_ref[...]
    lane = lax.broadcasted_iota(jnp.int32, (128, 128), 1)
    for b in range(blocks):
        reads[b].wait()
        total = jnp.zeros((128, 128), F32)
        for e in range(experts):
            row = jnp.max(jnp.abs(taken[b, e]), axis=1, keepdims=True)
            total = jnp.where(lane == e, row, total)
        out_ref[:, pl.ds(128 * b, 128)] = total.T[:experts]


def local_maxima(w, router, gain):
    experts, rows, _ = w.shape
    blocks = rows // 128
    return pl.pallas_call(
        local_kernel,
        out_shape=jax.ShapeDtypeStruct((experts, rows + 128), F32),
        in_specs=[ANY, VMEM, VMEM],
        out_specs=VMEM,
        scratch_shapes=[pltpu.VMEM((blocks, experts, 128, 128), F32), pltpu.SemaphoreType.DMA((blocks,))],
        compiler_params=params(56),
        cost_estimate=cost(8 * 2**20, 2**16),
        name="local_maxima",
    )(w, router, gain)


def inverse_columns(scale_ref, inverse, slot, block):
    inverse[pl.ds(128 * slot, 128), :] = jnp.concatenate([1.0 / scale_ref[:, lanes(block)]] * 8, axis=0).T


def across_kernel(hops, f_ref, w_ref, scale_ref, *refs):
    outs, (taken, inverse, made, in_sems, out_sems) = refs[: len(hops)], refs[len(hops) :]
    count = taken.shape[1]
    f = f_ref[0]
    targets = [partner(f, 1, *hop) for hop in hops]
    reads = []
    for k, target in enumerate(targets):
        rows = pl.ds(pl.multiple_of(target * 64, 64), 64)
        reads.append(pltpu.make_async_copy(w_ref.at[pl.ds(0, count), rows, :], taken.at[k], in_sems.at[k]))
        reads[-1].start()
    for dx in sorted({dx for dx, _ in hops}):
        inverse_columns(scale_ref, inverse, dx, partner(f, 1, dx, 0) // 2)
    writes = []
    for k, target in enumerate(targets):
        columns = inverse[pl.ds(pl.multiple_of(hops[k][0] * 128 + target % 2 * 64, 64), 64), :]
        reads[k].wait()
        for e in range(count):
            made[k, e] = (taken[k, e] * columns[:, e : e + 1]).astype(BF16)
        writes.append(pltpu.make_async_copy(made.at[k], outs[k], out_sems.at[k]))
        writes[-1].start()
    for write in writes:
        write.wait()


def across_pieces(hops, f, w, scale, count):
    n = len(hops)
    return pl.pallas_call(
        functools.partial(across_kernel, hops),
        out_shape=[jax.ShapeDtypeStruct((count, 64, 128), BF16)] * n,
        in_specs=[SMEM, ANY, VMEM],
        out_specs=[ANY] * n,
        scratch_shapes=[
            pltpu.VMEM((n, count, 64, 128), F32),
            pltpu.VMEM((512, 128), F32),
            pltpu.VMEM((n, count, 64, 128), BF16),
            pltpu.SemaphoreType.DMA((n,)),
            pltpu.SemaphoreType.DMA((n,)),
        ],
        compiler_params=params(56),
        cost_estimate=cost(n * 2**19, n * 2**18),
        name="across_pieces",
    )(f, w, scale)


def plane_kernel(f_ref, y_ref, w_ref, scale_ref, relay_ref, near_ref, r1_ref, r2_ref, r3_ref, *refs):
    outs, (final_ref, router_ref), (taken, inverse, made, in_sems, out_sems) = refs[:7], refs[7:9], refs[9:]
    experts, early = w_ref.shape[0], relay_ref.shape[0]
    f, y = f_ref[0], y_ref[0]
    reads = []
    for k, (dx, dc) in enumerate(HOPS):
        rows = pl.ds(pl.multiple_of(partner(f, 0, dx, dc) * 64, 64), 64)
        reads.append(pltpu.make_async_copy(w_ref.at[:, rows, :], taken.at[k], in_sems.at[k]))
        reads[-1].start()
    for dx in range(4):
        inverse_columns(scale_ref, inverse, dx, partner(f, 0, dx, 0) // 2)
    for k, (dx, dc) in enumerate(HOPS):
        target = partner(f, 0, dx, dc)
        local = pl.ds(pl.multiple_of(target % 8 * 64, 64), 64)
        columns = inverse[pl.ds(pl.multiple_of(dx * 128 + target % 2 * 64, 64), 64), :]
        reads[k].wait()
        for e in range(experts):
            made[k, e] = (taken[k, e] * columns[:, e : e + 1]).astype(BF16)
        for q in range(early):
            e = experts - early + q
            made[k, experts + q] = (relay_ref[q, local, :] * columns[:, e : e + 1]).astype(BF16)
        for plane in range(2):
            for dy, piece in enumerate((near_ref, r1_ref, r2_ref, r3_ref)):
                at = pl.multiple_of((y - dy + 4) % 4 * 16, 16)
                made[k, experts + early + plane, pl.ds(at, 16), :] = piece[plane]
    other = f + 8 - f // 8 * 16
    here = made.at[0]
    writes = [
        pltpu.make_async_copy(here.at[pl.ds(0, experts)], final_ref.at[:, :, lanes(f)], out_sems.at[0]),
        pltpu.make_async_copy(here.at[experts + early], router_ref.at[:, lanes(f)], out_sems.at[8]),
        pltpu.make_async_copy(here.at[experts + early + 1], router_ref.at[:, lanes(other)], out_sems.at[9]),
    ]
    if early:
        writes.append(
            pltpu.make_async_copy(
                here.at[pl.ds(experts, early)],
                final_ref.at[pl.ds(experts - early, early), :, lanes(other)],
                out_sems.at[10],
            )
        )
    for k in range(1, 8):
        writes.append(pltpu.make_async_copy(made.at[k], outs[k - 1], out_sems.at[k]))
    for write in writes:
        write.start()
    for write in writes:
        write.wait()


def plane_pieces(f, y, w, scale, relay, near, *received):
    experts, _, _ = w.shape
    blocks = experts + relay.shape[0] + 2
    return pl.pallas_call(
        plane_kernel,
        out_shape=[jax.ShapeDtypeStruct((blocks, 64, 128), BF16)] * 7
        + [jax.ShapeDtypeStruct((experts, 64, 2048), BF16), jax.ShapeDtypeStruct((64, 2048), BF16)],
        in_specs=[SMEM, SMEM, ANY] + [VMEM] * 6,
        out_specs=[ANY] * 9,
        scratch_shapes=[
            pltpu.VMEM((8, experts, 64, 128), F32),
            pltpu.VMEM((512, 128), F32),
            pltpu.VMEM((8, blocks, 64, 128), BF16),
            pltpu.SemaphoreType.DMA((8,)),
            pltpu.SemaphoreType.DMA((11,)),
        ],
        compiler_params=params(56),
        cost_estimate=cost(5 * 2**20, 3 * 2**20),
        name="plane_pieces",
    )(f, y, w, scale, relay, near, *received)


def place_across_kernel(hop, f_ref, piece_ref, _, final_ref, sem):
    source = partner(f_ref[0], 1, 4 - hop[0], hop[1])
    copy = pltpu.make_async_copy(piece_ref, final_ref.at[pl.ds(0, piece_ref.shape[0]), :, lanes(source)], sem)
    copy.start()
    copy.wait()


def place_across(hop, f, piece, final):
    return pl.pallas_call(
        functools.partial(place_across_kernel, hop),
        out_shape=jax.ShapeDtypeStruct(final.shape, final.dtype),
        in_specs=[SMEM, VMEM, ANY],
        out_specs=ANY,
        scratch_shapes=[pltpu.SemaphoreType.DMA],
        input_output_aliases={2: 0},
        compiler_params=params(2),
        cost_estimate=cost(2**18, 2**18),
        name="place_across",
    )(f, piece, final)


def place_plane_kernel(hop, early, f_ref, piece_ref, _, __, final_ref, router_ref, sems):
    experts = final_ref.shape[0]
    source = partner(f_ref[0], 0, 4 - hop[0], hop[1])
    other = source + 8 - source // 8 * 16
    copies = [
        pltpu.make_async_copy(piece_ref.at[pl.ds(0, experts)], final_ref.at[:, :, lanes(source)], sems.at[0]),
        pltpu.make_async_copy(piece_ref.at[experts + early], router_ref.at[:, lanes(source)], sems.at[1]),
        pltpu.make_async_copy(piece_ref.at[experts + early + 1], router_ref.at[:, lanes(other)], sems.at[2]),
    ]
    if early:
        copies.append(
            pltpu.make_async_copy(
                piece_ref.at[pl.ds(experts, early)],
                final_ref.at[pl.ds(experts - early, early), :, lanes(other)],
                sems.at[3],
            )
        )
    for copy in copies:
        copy.start()
    for copy in copies:
        copy.wait()


def place_plane(hop, early, f, piece, final, router):
    return pl.pallas_call(
        functools.partial(place_plane_kernel, hop, early),
        out_shape=[jax.ShapeDtypeStruct(final.shape, BF16), jax.ShapeDtypeStruct(router.shape, BF16)],
        in_specs=[SMEM, VMEM, ANY, ANY],
        out_specs=[ANY, ANY],
        scratch_shapes=[pltpu.SemaphoreType.DMA((4,))],
        input_output_aliases={2: 0, 3: 1},
        compiler_params=params(2),
        cost_estimate=cost(2**18, 2**18),
        name="place_plane",
    )(f, piece, final, router)


def send(piece, dz, dx, dc):
    return lax.ppermute(piece, "fsdp", route(dz, dx, dc))


def served(master_down, router_weight, router_gain):
    experts, rows, _ = master_down.shape
    position = lax.axis_index("fsdp")
    f = position.reshape(1)
    y = lax.axis_index("ep").reshape(1)

    local = local_maxima(master_down, router_weight.T, router_gain.reshape(1, -1))
    peer = send(local, 1, 0, 0)
    early = lax.dynamic_slice(
        master_down, (experts - EARLY, (1 - position // 8) * 512, 0), (EARLY, 512, 128)
    )
    relay = send(early, 1, 0, 0)
    scale = jnp.maximum(local[:, :rows], peer[:, :rows])
    near = jnp.stack([local[:, rows:], peer[:, rows:]]).astype(BF16)
    scale = jnp.maximum(scale, send(scale, 0, 0, 1))
    scale = functools.reduce(jnp.maximum, [scale] + [send(scale, 0, dx, 0) for dx in (1, 3, 2)])

    pieces = across_pieces(HOPS[:1], f, master_down, scale, experts - EARLY)
    pieces += across_pieces(HOPS[1:], f, master_down, scale, experts - EARLY)
    across = [send(piece, 1, *HOPS[k]) for k, piece in enumerate(pieces)]
    received = []
    for d in (1, 2, 3):
        received.append(lax.ppermute(near, "ep", [(i, (i + d) % 4) for i in range(4)]))
    *pieces, final, router = plane_pieces(f, y, master_down, scale, relay, near, *received)
    plane = [send(piece, 0, *HOPS[k + 1]) for k, piece in enumerate(pieces)]
    for k in range(2):
        final = place_across(HOPS[k], f, across[k], final)
    for k in range(7):
        final, router = place_plane(HOPS[k + 1], EARLY, f, plane[k], final, router)
    for k in range(2, 8):
        final = place_across(HOPS[k], f, across[k], final)
    own = lax.dynamic_slice_in_dim(scale, position * 64, 64, axis=1)
    return final, own, router.T


def solution(mesh):
    return jax.shard_map(
        served,
        mesh=mesh,
        in_specs=(
            P(("trial", "ep"), None, "fsdp"),
            P(("trial", "fsdp"), "ep"),
            P(("trial", "fsdp")),
        ),
        out_specs=(P(("trial", "ep"), "fsdp", None), P(("trial", "ep"), "fsdp"), P("trial", None)),
        check_vma=False,
    )
```

```python
import functools

import jax
import jax.numpy as jnp
from jax import lax
from jax.experimental import pallas as pl
from jax.experimental.pallas import tpu as pltpu
from jax.sharding import PartitionSpec as P


RELAY = 7
EARLY = 1
BF16, F32 = jnp.bfloat16, jnp.float32
ANY = pl.BlockSpec(memory_space=pl.ANY)
VMEM = pl.BlockSpec(memory_space=pltpu.VMEM)
SMEM = pl.BlockSpec(memory_space=pltpu.SMEM)
HOPS = [(dx, dc) for dx in range(4) for dc in range(2)]


def params(mebibytes):
    return pltpu.CompilerParams(vmem_limit_bytes=int(mebibytes * 2**20))


def cost(read, written):
    return pl.CostEstimate(flops=(read + written) * 4, bytes_accessed=read + written, transcendentals=0)


def route(dz, dx, dc):
    pairs = []
    for f in range(16):
        z, x, c = f // 8, f // 2 % 4, f % 2
        pairs.append((f, (z ^ dz) * 8 + (x + dx) % 4 * 2 + (c ^ dc)))
    return pairs


def partner(f, dz, dx, dc):
    z, x, c = f // 8, f // 2 % 4, f % 2
    z = z if dz == 0 else 1 - z
    c = c if dc == 0 else 1 - c
    return z * 8 + (x + dx) % 4 * 2 + c


def lanes(position):
    return pl.ds(pl.multiple_of(position * 128, 128), 128)


def local_kernel(w_ref, out_ref, taken, sems):
    blocks, experts = taken.shape[:2]
    reads = []
    for b in range(blocks):
        reads.append(pltpu.make_async_copy(w_ref.at[:, pl.ds(128 * b, 128), :], taken.at[b], sems.at[b]))
        reads[-1].start()
    lane = lax.broadcasted_iota(jnp.int32, (128, 128), 1)
    for b in range(blocks):
        reads[b].wait()
        total = jnp.zeros((128, 128), F32)
        for e in range(experts):
            row = jnp.max(jnp.abs(taken[b, e]), axis=1, keepdims=True)
            total = jnp.where(lane == e, row, total)
        out_ref[:, pl.ds(128 * b, 128)] = total.T[:experts]


def local_maxima(w):
    experts, rows, _ = w.shape
    blocks = rows // 128
    return pl.pallas_call(
        local_kernel,
        out_shape=jax.ShapeDtypeStruct((experts, rows), F32),
        in_specs=[ANY],
        out_specs=VMEM,
        scratch_shapes=[pltpu.VMEM((blocks, experts, 128, 128), F32), pltpu.SemaphoreType.DMA((blocks,))],
        compiler_params=params(50),
        cost_estimate=cost(8 * 2**20, 2**16),
        name="local_maxima",
    )(w)


def inverse_columns(scale_ref, inverse, slot, block):
    inverse[pl.ds(128 * slot, 128), :] = jnp.concatenate([1.0 / scale_ref[:, lanes(block)]] * 8, axis=0).T


def chunk_kernel(f_ref, w_ref, scale_ref, out_ref, taken, inverse, made, in_sems, out_sems):
    count = taken.shape[1]
    plane = 1 - f_ref[0] // 8
    reads = []
    for b in range(4):
        rows = pl.ds(pl.multiple_of(plane * 512 + 128 * b, 128), 128)
        reads.append(pltpu.make_async_copy(w_ref.at[pl.ds(0, count), rows, :], taken.at[b], in_sems.at[b]))
        reads[-1].start()
    writes = []
    for b in range(4):
        inverse_columns(scale_ref, inverse, b, 4 * plane + b)
        columns = inverse[pl.ds(128 * b, 128), :]
        reads[b].wait()
        for e in range(count):
            made[b, e] = (taken[b, e] * columns[:, e : e + 1]).astype(BF16)
        writes.append(pltpu.make_async_copy(made.at[b], out_ref.at[:, pl.ds(128 * b, 128), :], out_sems.at[b]))
        writes[-1].start()
    for write in writes:
        write.wait()


def chunk(f, w, scale, count):
    return pl.pallas_call(
        chunk_kernel,
        out_shape=jax.ShapeDtypeStruct((count, 512, 128), BF16),
        in_specs=[SMEM, ANY, VMEM],
        out_specs=ANY,
        scratch_shapes=[
            pltpu.VMEM((4, count, 128, 128), F32),
            pltpu.VMEM((512, 128), F32),
            pltpu.VMEM((4, count, 128, 128), BF16),
            pltpu.SemaphoreType.DMA((4,)),
            pltpu.SemaphoreType.DMA((4,)),
        ],
        compiler_params=params(50),
        cost_estimate=cost(4 * 2**20, 2 * 2**20),
        name="chunk",
    )(f, w, scale)


def split_kernel(f_ref, chunk_ref, _, *refs):
    outs, final_ref, sems = refs[:7], refs[7], refs[8]
    f = f_ref[0]
    copies = []
    for k, hop in enumerate(HOPS):
        rows = pl.ds(pl.multiple_of(partner(f, 0, *hop) % 8 * 64, 64), 64)
        piece = chunk_ref.at[:, rows, :]
        if k == 0:
            target = final_ref.at[pl.ds(0, chunk_ref.shape[0]), :, lanes(partner(f, 1, 0, 0))]
        else:
            target = outs[k - 1]
        copies.append(pltpu.make_async_copy(piece, target, sems.at[k]))
        copies[-1].start()
    for copy in copies:
        copy.wait()


def split(f, chunk, final):
    count = chunk.shape[0]
    return pl.pallas_call(
        split_kernel,
        out_shape=[jax.ShapeDtypeStruct((count, 64, 128), BF16)] * 7
        + [jax.ShapeDtypeStruct(final.shape, BF16)],
        in_specs=[SMEM, VMEM, ANY],
        out_specs=[ANY] * 8,
        scratch_shapes=[pltpu.SemaphoreType.DMA((8,))],
        input_output_aliases={2: 7},
        compiler_params=params(50),
        cost_estimate=cost(2**20, 2**20),
        name="split",
    )(f, chunk, final)


def across_kernel(hops, first, f_ref, w_ref, scale_ref, *refs):
    outs, (taken, inverse, made, in_sems, out_sems) = refs[: len(hops)], refs[len(hops) :]
    count = taken.shape[1]
    f = f_ref[0]
    targets = [partner(f, 1, *hop) for hop in hops]
    reads = []
    for k, target in enumerate(targets):
        rows = pl.ds(pl.multiple_of(target * 64, 64), 64)
        reads.append(pltpu.make_async_copy(w_ref.at[pl.ds(first, count), rows, :], taken.at[k], in_sems.at[k]))
        reads[-1].start()
    for dx in sorted({dx for dx, _ in hops}):
        inverse_columns(scale_ref, inverse, dx, partner(f, 1, dx, 0) // 2)
    writes = []
    for k, target in enumerate(targets):
        columns = inverse[pl.ds(pl.multiple_of(hops[k][0] * 128 + target % 2 * 64, 64), 64), :]
        reads[k].wait()
        for e in range(count):
            made[k, e] = (taken[k, e] * columns[:, first + e : first + e + 1]).astype(BF16)
        writes.append(pltpu.make_async_copy(made.at[k], outs[k], out_sems.at[k]))
        writes[-1].start()
    for write in writes:
        write.wait()


def across_pieces(hops, f, w, scale, first, count):
    n = len(hops)
    return pl.pallas_call(
        functools.partial(across_kernel, hops, first),
        out_shape=[jax.ShapeDtypeStruct((count, 64, 128), BF16)] * n,
        in_specs=[SMEM, ANY, VMEM],
        out_specs=[ANY] * n,
        scratch_shapes=[
            pltpu.VMEM((n, count, 64, 128), F32),
            pltpu.VMEM((512, 128), F32),
            pltpu.VMEM((n, count, 64, 128), BF16),
            pltpu.SemaphoreType.DMA((n,)),
            pltpu.SemaphoreType.DMA((n,)),
        ],
        compiler_params=params(50),
        cost_estimate=cost(n * 2**19, n * 2**18),
        name="across_pieces",
    )(f, w, scale)


def plane_kernel(f_ref, y_ref, w_ref, scale_ref, relay_ref, near_ref, r1_ref, r2_ref, r3_ref, *refs):
    outs, (final_ref, router_ref), (taken, inverse, made, in_sems, out_sems) = refs[:7], refs[7:9], refs[9:]
    experts, early = w_ref.shape[0], EARLY
    f, y = f_ref[0], y_ref[0]
    reads = []
    for k, (dx, dc) in enumerate(HOPS):
        rows = pl.ds(pl.multiple_of(partner(f, 0, dx, dc) * 64, 64), 64)
        reads.append(pltpu.make_async_copy(w_ref.at[:, rows, :], taken.at[k], in_sems.at[k]))
        reads[-1].start()
    for dx in range(4):
        inverse_columns(scale_ref, inverse, dx, partner(f, 0, dx, 0) // 2)
    for k, (dx, dc) in enumerate(HOPS):
        target = partner(f, 0, dx, dc)
        columns = inverse[pl.ds(pl.multiple_of(dx * 128 + target % 2 * 64, 64), 64), :]
        reads[k].wait()
        for e in range(experts):
            made[k, e] = (taken[k, e] * columns[:, e : e + 1]).astype(BF16)
        for q in range(early):
            e = experts - early + q
            made[k, experts + q] = (relay_ref[pl.ds(pl.multiple_of(512 * q + target % 8 * 64, 64), 64), :] * columns[:, e : e + 1]).astype(BF16)
        for plane in range(2):
            for dy, piece in enumerate((near_ref, r1_ref, r2_ref, r3_ref)):
                at = pl.multiple_of((y - dy + 4) % 4 * 16, 16)
                made[k, experts + early + plane, pl.ds(at, 16), :] = piece[plane]
    other = f + 8 - f // 8 * 16
    here = made.at[0]
    writes = [
        pltpu.make_async_copy(here.at[pl.ds(0, experts)], final_ref.at[:, :, lanes(f)], out_sems.at[0]),
        pltpu.make_async_copy(here.at[experts + early], router_ref.at[:, lanes(f)], out_sems.at[8]),
        pltpu.make_async_copy(here.at[experts + early + 1], router_ref.at[:, lanes(other)], out_sems.at[9]),
    ]
    if early:
        writes.append(
            pltpu.make_async_copy(
                here.at[pl.ds(experts, early)],
                final_ref.at[pl.ds(experts - early, early), :, lanes(other)],
                out_sems.at[10],
            )
        )
    for k in range(1, 8):
        writes.append(pltpu.make_async_copy(made.at[k], outs[k - 1], out_sems.at[k]))
    for write in writes:
        write.start()
    for write in writes:
        write.wait()


def plane_pieces(f, y, w, scale, relay, near, *received):
    experts, _, _ = w.shape
    blocks = experts + EARLY + 2
    return pl.pallas_call(
        plane_kernel,
        out_shape=[jax.ShapeDtypeStruct((blocks, 64, 128), BF16)] * 7
        + [jax.ShapeDtypeStruct((experts, 64, 2048), BF16), jax.ShapeDtypeStruct((64, 2048), BF16)],
        in_specs=[SMEM, SMEM, ANY] + [VMEM] * 6,
        out_specs=[ANY] * 9,
        scratch_shapes=[
            pltpu.VMEM((8, experts, 64, 128), F32),
            pltpu.VMEM((512, 128), F32),
            pltpu.VMEM((8, blocks, 64, 128), BF16),
            pltpu.SemaphoreType.DMA((8,)),
            pltpu.SemaphoreType.DMA((11,)),
        ],
        compiler_params=params(50),
        cost_estimate=cost(5 * 2**20, 3 * 2**20),
        name="plane_pieces",
    )(f, y, w, scale, relay, near, *received)


def place_far_kernel(hop, first, f_ref, piece_ref, _, final_ref, sem):
    dx, dc = hop
    source = partner(f_ref[0], 1, 4 - dx, dc)
    experts = pl.ds(first, piece_ref.shape[0])
    copy = pltpu.make_async_copy(piece_ref, final_ref.at[experts, :, lanes(source)], sem)
    copy.start()
    copy.wait()


def place_far(hop, first, f, piece, final):
    return pl.pallas_call(
        functools.partial(place_far_kernel, hop, first),
        out_shape=jax.ShapeDtypeStruct(final.shape, final.dtype),
        in_specs=[SMEM, VMEM, ANY],
        out_specs=ANY,
        scratch_shapes=[pltpu.SemaphoreType.DMA],
        input_output_aliases={2: 0},
        compiler_params=params(2),
        cost_estimate=cost(2**18, 2**18),
        name="place_far",
    )(f, piece, final)


def place_plane_kernel(hop, early, f_ref, piece_ref, _, __, final_ref, router_ref, sems):
    experts = final_ref.shape[0]
    source = partner(f_ref[0], 0, 4 - hop[0], hop[1])
    other = source + 8 - source // 8 * 16
    copies = [
        pltpu.make_async_copy(piece_ref.at[pl.ds(0, experts)], final_ref.at[:, :, lanes(source)], sems.at[0]),
        pltpu.make_async_copy(piece_ref.at[experts + early], router_ref.at[:, lanes(source)], sems.at[1]),
        pltpu.make_async_copy(piece_ref.at[experts + early + 1], router_ref.at[:, lanes(other)], sems.at[2]),
    ]
    if early:
        copies.append(
            pltpu.make_async_copy(
                piece_ref.at[pl.ds(experts, early)],
                final_ref.at[pl.ds(experts - early, early), :, lanes(other)],
                sems.at[3],
            )
        )
    for copy in copies:
        copy.start()
    for copy in copies:
        copy.wait()


def place_plane(hop, early, f, piece, final, router):
    return pl.pallas_call(
        functools.partial(place_plane_kernel, hop, early),
        out_shape=[jax.ShapeDtypeStruct(final.shape, BF16), jax.ShapeDtypeStruct(router.shape, BF16)],
        in_specs=[SMEM, VMEM, ANY, ANY],
        out_specs=[ANY, ANY],
        scratch_shapes=[pltpu.SemaphoreType.DMA((4,))],
        input_output_aliases={2: 0, 3: 1},
        compiler_params=params(2),
        cost_estimate=cost(2**18, 2**18),
        name="place_plane",
    )(f, piece, final, router)


def send(piece, dz, dx, dc):
    return lax.ppermute(piece, "fsdp", route(dz, dx, dc))


def served(master_down, router_weight, router_gain):
    experts, _, _ = master_down.shape
    direct = experts - RELAY - EARLY
    position = lax.axis_index("fsdp")
    f = position.reshape(1)
    y = lax.axis_index("ep").reshape(1)

    scale = local_maxima(master_down)
    peer = send(scale, 1, 0, 0)
    product = router_weight.T * router_gain.reshape(1, -1)
    early = lax.dynamic_slice(
        master_down, (experts - EARLY, (1 - position // 8) * 512, 0), (EARLY, 512, 128)
    )
    early = jnp.concatenate([early.reshape(EARLY * 512, 128), product])
    relay = send(early, 1, 0, 0)
    scale = jnp.maximum(scale, peer)
    scale = jnp.maximum(scale, send(scale, 0, 0, 1))
    scale = functools.reduce(jnp.maximum, [scale] + [send(scale, 0, dx, 0) for dx in (1, 3, 2)])

    forward = send(chunk(f, master_down, scale, RELAY), 1, 0, 0)
    near = jnp.stack([product, relay[EARLY * 512 :]]).astype(BF16)
    received = []
    for d in (1, 2, 3):
        received.append(lax.ppermute(near, "ep", [(i, (i + d) % 4) for i in range(4)]))
    *pieces, final, router = plane_pieces(f, y, master_down, scale, relay, near, *received)
    plane = [send(piece, 0, *HOPS[k + 1]) for k, piece in enumerate(pieces)]
    pieces = across_pieces(HOPS, f, master_down, scale, RELAY, direct)
    across = [send(piece, 1, *HOPS[k]) for k, piece in enumerate(pieces)]
    *pieces, final = split(f, forward, final)
    relayed = [send(piece, 0, *HOPS[k + 1]) for k, piece in enumerate(pieces)]

    for k in range(7):
        final, router = place_plane(HOPS[k + 1], EARLY, f, plane[k], final, router)
    for k in range(7):
        final = place_far(HOPS[k + 1], 0, f, relayed[k], final)
    for k in range(8):
        final = place_far(HOPS[k], RELAY, f, across[k], final)
    own = lax.dynamic_slice_in_dim(scale, position * 64, 64, axis=1)
    return final, own, router.T


def solution(mesh):
    return jax.shard_map(
        served,
        mesh=mesh,
        in_specs=(
            P(("trial", "ep"), None, "fsdp"),
            P(("trial", "fsdp"), "ep"),
            P(("trial", "fsdp")),
        ),
        out_specs=(P(("trial", "ep"), "fsdp", None), P(("trial", "ep"), "fsdp"), P("trial", None)),
        check_vma=False,
    )
```

```python
import functools

import jax
import jax.numpy as jnp
from jax import lax
from jax.experimental import pallas as pl
from jax.experimental.pallas import tpu as pltpu
from jax.sharding import PartitionSpec as P


RELAY = 7
EARLY = 1
BF16, F32 = jnp.bfloat16, jnp.float32
ANY = pl.BlockSpec(memory_space=pl.ANY)
VMEM = pl.BlockSpec(memory_space=pltpu.VMEM)
SMEM = pl.BlockSpec(memory_space=pltpu.SMEM)


def params(mebibytes):
    return pltpu.CompilerParams(vmem_limit_bytes=mebibytes * 2**20)


def cost(read, written):
    return pl.CostEstimate(flops=(read + written) * 4, bytes_accessed=read + written, transcendentals=0)


def array(*shape, kind=BF16):
    return jax.ShapeDtypeStruct(shape, kind)


def span(start, size):
    return pl.ds(pl.multiple_of(start, size), size)


def lanes(position):
    return span(position * 128, 128)


def route(dz, dx, dc):
    pairs = []
    for f in range(16):
        z, x, c = f // 8, f // 2 % 4, f % 2
        pairs.append((f, (z ^ dz) * 8 + (x + dx) % 4 * 2 + (c ^ dc)))
    return pairs


def send(piece, dz, dx, dc):
    return lax.ppermute(piece, "fsdp", route(dz, dx, dc))


def chip(f, dz, dx):
    z = f // 8 if dz == 0 else 1 - f // 8
    return z * 4 + (f // 2 + dx) % 4


def run(copies):
    for copy in copies:
        copy.start()
    for copy in copies:
        copy.wait()


def parts(experts):
    return (0, RELAY), (RELAY, experts - RELAY - EARLY), (experts - EARLY, EARLY)


def local_kernel(f_ref, w_ref, out_ref, *refs):
    swap_refs, (taken, in_sems, out_sems) = refs[:3], refs[3:]
    blocks, experts = taken.shape[:2]
    away = 1 - f_ref[0] % 2
    reads = []
    for b in range(blocks):
        reads.append(pltpu.make_async_copy(w_ref.at[:, pl.ds(128 * b, 128), :], taken.at[b], in_sems.at[b]))
        reads[-1].start()
    lane = lax.broadcasted_iota(jnp.int32, (128, 128), 1)
    writes = []
    for b in range(blocks):
        reads[b].wait()
        for k, ((first, count), target) in enumerate(zip(parts(experts), swap_refs)):
            rows = taken.at[b, pl.ds(first, count), span(64 * away, 64), :]
            writes.append(
                pltpu.make_async_copy(rows, target.at[:, pl.ds(64 * b, 64), :], out_sems.at[3 * b + k])
            )
            writes[-1].start()
        total = jnp.zeros((128, 128), F32)
        for e in range(experts):
            row = jnp.max(jnp.abs(taken[b, e]), axis=1, keepdims=True)
            total = jnp.where(lane == e, row, total)
        out_ref[:, pl.ds(128 * b, 128)] = total.T[:experts]
    for write in writes:
        write.wait()


def local_maxima(f, w):
    experts, rows, _ = w.shape
    blocks = rows // 128
    return pl.pallas_call(
        local_kernel,
        out_shape=[
            array(experts, rows, kind=F32),
            *(array(count, rows // 2, 128, kind=F32) for _, count in parts(experts)),
        ],
        in_specs=[SMEM, ANY],
        out_specs=[VMEM, ANY, ANY, ANY],
        scratch_shapes=[
            pltpu.VMEM((blocks, experts, 128, 128), F32),
            pltpu.SemaphoreType.DMA((blocks,)),
            pltpu.SemaphoreType.DMA((3 * blocks,)),
        ],
        compiler_params=params(50),
        cost_estimate=cost(8 * 2**20, 4 * 2**20),
        name="local_maxima",
    )(f, w)


def inverse_columns(scale_ref, inverse, slot, block):
    inverse[pl.ds(128 * slot, 128), :] = jnp.concatenate([1.0 / scale_ref[:, lanes(block)]] * 8, axis=0).T


def far_kernel(plan, f_ref, w_ref, theirs_ref, scale_ref, *refs):
    first, count, whole = plan
    outs, (taken, inverse, made, in_sems, out_sems) = refs[:-5], refs[-5:]
    f = f_ref[0]
    core = f % 2
    experts = pl.ds(first, count)
    reads = []
    for dx in range(4):
        q = 4 * (1 - f // 8) + dx if whole else chip(f, 1, dx)
        own = w_ref.at[experts, span(128 * q + 64 * core, 64), :]
        theirs = theirs_ref.at[:, span(64 * q, 64), :]
        for k, rows in enumerate((own, theirs)):
            reads.append(
                pltpu.make_async_copy(rows, taken.at[dx, pl.ds(k * count, count)], in_sems.at[2 * dx + k])
            )
            reads[-1].start()
    writes = []
    for dx in range(4):
        q = 4 * (1 - f // 8) + dx if whole else chip(f, 1, dx)
        inverse_columns(scale_ref, inverse, dx, q)
        columns = inverse[span(128 * dx + 64 * core, 64), :]
        for k in range(2):
            reads[2 * dx + k].wait()
            for e in range(count):
                at, lane = k * count + e, first + e
                made[dx, at] = (taken[dx, at] * columns[:, lane : lane + 1]).astype(BF16)
        target = outs[0].at[:, pl.ds(64 * dx, 64), :] if whole else outs[dx]
        writes.append(pltpu.make_async_copy(made.at[dx], target, out_sems.at[dx]))
        writes[-1].start()
    for write in writes:
        write.wait()


def far_pieces(f, w, theirs, scale, first, count, whole):
    outs = [array(2 * count, 256, 128)] if whole else [array(2 * count, 64, 128)] * 4
    return pl.pallas_call(
        functools.partial(far_kernel, (first, count, whole)),
        out_shape=outs,
        in_specs=[SMEM, ANY, ANY, VMEM],
        out_specs=[ANY] * len(outs),
        scratch_shapes=[
            pltpu.VMEM((4, 2 * count, 64, 128), F32),
            pltpu.VMEM((512, 128), F32),
            pltpu.VMEM((4, 2 * count, 64, 128), BF16),
            pltpu.SemaphoreType.DMA((8,)),
            pltpu.SemaphoreType.DMA((4,)),
        ],
        compiler_params=params(50),
        cost_estimate=cost(2 * 2**20, 2**20),
        name="far_pieces",
    )(f, w, theirs, scale)


def near_kernel(f_ref, y_ref, w_ref, scale_ref, relay_ref, *refs):
    rows_refs, theirs_refs, refs = refs[:4], refs[4:7], refs[7:]
    outs, (final_ref, router_ref), (taken, inverse, made, in_sems, out_sems) = refs[:3], refs[3:5], refs[5:]
    experts = w_ref.shape[0]
    late = experts - EARLY
    f, y = f_ref[0], y_ref[0]
    core = f % 2
    reads = []
    for dx in range(4):
        q = chip(f, 0, dx)
        own = w_ref.at[:, span(128 * q + 64 * core, 64), :]
        rows = [(own, 0, experts)]
        for (first, count), theirs_ref in zip(parts(experts), theirs_refs):
            rows.append((theirs_ref.at[:, span(64 * q, 64), :], experts + first, count))
        for k, (piece, at, size) in enumerate(rows):
            reads.append(pltpu.make_async_copy(piece, taken.at[dx, pl.ds(at, size)], in_sems.at[4 * dx + k]))
            reads[-1].start()
    for dx in range(4):
        q = chip(f, 0, dx)
        inverse_columns(scale_ref, inverse, dx, q)
        columns = inverse[span(128 * dx + 64 * core, 64), :]
        for k in range(4):
            reads[4 * dx + k].wait()
        for k in range(2):
            for e in range(experts):
                at = k * experts + e
                made[dx, at] = (taken[dx, at] * columns[:, e : e + 1]).astype(BF16)
            for j in range(EARLY):
                rows = relay_ref[span(256 * (k * EARLY + j) + 64 * (q % 4), 64), :]
                lane = late + j
                made[dx, 2 * experts + k * EARLY + j] = (rows * columns[:, lane : lane + 1]).astype(BF16)
        for k in range(4):
            for dy, piece in enumerate(rows_refs):
                made[dx, 2 * experts + 2 * EARLY + k, span((y - dy + 4) % 4 * 16, 16), :] = piece[k]
    copies = [pltpu.make_async_copy(made.at[dx], outs[dx - 1], out_sems.at[dx]) for dx in (1, 2, 3)]
    copies += near_copies(f, f // 2, made.at[0], final_ref, router_ref, out_sems, 4)
    run(copies)


def near_copies(f, source, piece, final_ref, router_ref, sems, at):
    experts = final_ref.shape[0]
    core = f % 2
    across = (source + 4) % 8
    early = pl.ds(experts - EARLY, EARLY)
    copies = []
    for k in range(2):
        side = core if k == 0 else 1 - core
        copies.append((piece.at[pl.ds(k * experts, experts)], final_ref.at[:, :, lanes(2 * source + side)]))
        copies.append(
            (
                piece.at[pl.ds(2 * experts + k * EARLY, EARLY)],
                final_ref.at[early, :, lanes(2 * across + side)],
            )
        )
        for j, q in enumerate((source, across)):
            copies.append(
                (piece.at[2 * experts + 2 * EARLY + 2 * k + j], router_ref.at[:, lanes(2 * q + side)])
            )
    return [pltpu.make_async_copy(a, b, sems.at[at + k]) for k, (a, b) in enumerate(copies)]


def near_pieces(f, y, w, scale, relay, rows, theirs):
    experts = w.shape[0]
    blocks = 2 * experts + 2 * EARLY + 4
    return pl.pallas_call(
        near_kernel,
        out_shape=[array(blocks, 64, 128)] * 3 + [array(experts, 64, 2048), array(64, 2048)],
        in_specs=[SMEM, SMEM, ANY] + [VMEM] * 6 + [ANY] * 3,
        out_specs=[ANY] * 5,
        scratch_shapes=[
            pltpu.VMEM((4, 2 * experts, 64, 128), F32),
            pltpu.VMEM((512, 128), F32),
            pltpu.VMEM((4, blocks, 64, 128), BF16),
            pltpu.SemaphoreType.DMA((16,)),
            pltpu.SemaphoreType.DMA((12,)),
        ],
        compiler_params=params(50),
        cost_estimate=cost(5 * 2**20, 3 * 2**20),
        name="near_pieces",
    )(f, y, w, scale, relay, *rows, *theirs)


def split_kernel(f_ref, chunk_ref, _, *refs):
    outs, final_ref, sems = refs[:3], refs[3], refs[4]
    f = f_ref[0]
    copies = []
    for dx in (1, 2, 3):
        rows = chunk_ref.at[:, span(64 * (chip(f, 0, dx) % 4), 64), :]
        copies.append(pltpu.make_async_copy(rows, outs[dx - 1], sems.at[dx - 1]))
    rows = chunk_ref.at[:, span(64 * (chip(f, 0, 0) % 4), 64), :]
    run(copies + far_copies(f, chip(f, 1, 0), 0, rows, final_ref, sems, 3))


def far_copies(f, source, first, piece, final_ref, sems, at):
    count = piece.shape[0] // 2
    copies = []
    for k in range(2):
        side = f % 2 if k == 0 else 1 - f % 2
        target = final_ref.at[pl.ds(first, count), :, lanes(2 * source + side)]
        copies.append(pltpu.make_async_copy(piece.at[pl.ds(k * count, count)], target, sems.at[at + k]))
    return copies


def split(f, chunk, final):
    return pl.pallas_call(
        split_kernel,
        out_shape=[array(chunk.shape[0], 64, 128)] * 3 + [array(*final.shape)],
        in_specs=[SMEM, VMEM, ANY],
        out_specs=[ANY] * 4,
        scratch_shapes=[pltpu.SemaphoreType.DMA((5,))],
        input_output_aliases={2: 3},
        compiler_params=params(50),
        cost_estimate=cost(2**20, 2**20),
        name="split",
    )(f, chunk, final)


def place_far_kernel(dx, first, f_ref, piece_ref, _, final_ref, sems):
    f = f_ref[0]
    run(far_copies(f, chip(f, 1, 4 - dx), first, piece_ref, final_ref, sems, 0))


def place_far(dx, first, f, piece, final):
    return pl.pallas_call(
        functools.partial(place_far_kernel, dx, first),
        out_shape=array(*final.shape),
        in_specs=[SMEM, VMEM, ANY],
        out_specs=ANY,
        scratch_shapes=[pltpu.SemaphoreType.DMA((2,))],
        input_output_aliases={2: 0},
        compiler_params=params(2),
        cost_estimate=cost(2**18, 2**18),
        name="place_far",
    )(f, piece, final)


def place_near_kernel(dx, f_ref, piece_ref, _, __, final_ref, router_ref, sems):
    f = f_ref[0]
    run(near_copies(f, chip(f, 0, 4 - dx), piece_ref, final_ref, router_ref, sems, 0))


def place_near(dx, f, piece, final, router):
    return pl.pallas_call(
        functools.partial(place_near_kernel, dx),
        out_shape=[array(*final.shape), array(*router.shape)],
        in_specs=[SMEM, VMEM, ANY, ANY],
        out_specs=[ANY, ANY],
        scratch_shapes=[pltpu.SemaphoreType.DMA((8,))],
        input_output_aliases={2: 0, 3: 1},
        compiler_params=params(2),
        cost_estimate=cost(2**19, 2**19),
        name="place_near",
    )(f, piece, final, router)


def served(w, router_weight, router_gain):
    experts, _, _ = w.shape
    position = lax.axis_index("fsdp")
    f = position.reshape(1)
    y = lax.axis_index("ep").reshape(1)
    far_plane = 1 - position // 8

    scale, swap, swap_direct, swap_early = local_maxima(f, w)
    theirs_early = send(swap_early, 0, 0, 1)
    peer = send(scale, 1, 0, 0)
    product = router_weight.T * router_gain.reshape(1, -1)
    own = lax.dynamic_slice(
        w.reshape(experts, 8, 2, 64, 128), (experts - EARLY, 4 * far_plane, position % 2, 0, 0), (EARLY, 4, 1, 64, 128)
    )
    other = lax.dynamic_slice(theirs_early, (0, 256 * far_plane, 0), (EARLY, 256, 128))
    early = jnp.concatenate([own.reshape(-1, 128), other.reshape(-1, 128), product])
    relay = send(early, 1, 0, 0)
    theirs = send(swap, 0, 0, 1)
    theirs_direct = send(swap_direct, 0, 0, 1)
    scale = jnp.maximum(scale, peer)
    scale = jnp.maximum(scale, send(scale, 0, 0, 1))
    scale = functools.reduce(jnp.maximum, [scale] + [send(scale, 0, dx, 0) for dx in (1, 3, 2)])

    (chunk,) = far_pieces(f, w, theirs, scale, 0, RELAY, True)
    forward = send(chunk, 1, 0, 0)
    near = jnp.stack([product, relay[2 * EARLY * 256 :]]).astype(BF16)
    near = jnp.concatenate([near, send(near, 0, 0, 1)])
    received = [near]
    for d in (1, 2, 3):
        received.append(lax.ppermute(near, "ep", [(i, (i + d) % 4) for i in range(4)]))
    *pieces, final, router = near_pieces(f, y, w, scale, relay, received, (theirs, theirs_direct, theirs_early))
    plane = [send(piece, 0, k + 1, 0) for k, piece in enumerate(pieces)]
    pieces = far_pieces(f, w, theirs_direct, scale, RELAY, experts - RELAY - EARLY, False)
    across = [send(piece, 1, k, 0) for k, piece in enumerate(pieces)]
    for k in range(3):
        final, router = place_near(k + 1, f, plane[k], final, router)
    *pieces, final = split(f, forward, final)
    relayed = [send(piece, 0, k + 1, 0) for k, piece in enumerate(pieces)]
    for k in range(3):
        final = place_far(k + 1, 0, f, relayed[k], final)
    for k in range(4):
        final = place_far(k, RELAY, f, across[k], final)
    own = lax.dynamic_slice_in_dim(scale, position * 64, 64, axis=1)
    return final, own, router.T


def solution(mesh):
    return jax.shard_map(
        served,
        mesh=mesh,
        in_specs=(
            P(("trial", "ep"), None, "fsdp"),
            P(("trial", "fsdp"), "ep"),
            P(("trial", "fsdp")),
        ),
        out_specs=(P(("trial", "ep"), "fsdp", None), P(("trial", "ep"), "fsdp"), P("trial", None)),
        check_vma=False,
    )
```

```python
import functools

import jax
import jax.numpy as jnp
from jax import lax
from jax.experimental import pallas as pl
from jax.experimental.pallas import tpu as pltpu
from jax.sharding import PartitionSpec as P


RELAY = 4
EARLY = 1
BF16, F32 = jnp.bfloat16, jnp.float32
ANY = pl.BlockSpec(memory_space=pl.ANY)
VMEM = pl.BlockSpec(memory_space=pltpu.VMEM)
SMEM = pl.BlockSpec(memory_space=pltpu.SMEM)


def params(mebibytes):
    return pltpu.CompilerParams(vmem_limit_bytes=mebibytes * 2**20)


def cost(read, written):
    return pl.CostEstimate(flops=(read + written) * 4, bytes_accessed=read + written, transcendentals=0)


def array(*shape, kind=BF16):
    return jax.ShapeDtypeStruct(shape, kind)


def span(start, size):
    return pl.ds(pl.multiple_of(start, size), size)


def lanes(position):
    return span(position * 128, 128)


def route(dz, dx, dc):
    pairs = []
    for f in range(16):
        z, x, c = f // 8, f // 2 % 4, f % 2
        pairs.append((f, (z ^ dz) * 8 + (x + dx) % 4 * 2 + (c ^ dc)))
    return pairs


def send(piece, dz, dx, dc):
    return lax.ppermute(piece, "fsdp", route(dz, dx, dc))


def chip(f, dz, dx):
    z = f // 8 if dz == 0 else 1 - f // 8
    return z * 4 + (f // 2 + dx) % 4


def run(copies):
    for copy in copies:
        copy.start()
    for copy in copies:
        copy.wait()


def parts(experts):
    return (0, RELAY), (RELAY, experts - RELAY - EARLY), (experts - EARLY, EARLY)


def local_kernel(f_ref, w_ref, out_ref, *refs):
    swap_refs, (taken, in_sems, out_sems) = refs[:2], refs[2:]
    blocks, experts = taken.shape[:2]
    away = 1 - f_ref[0] % 2
    reads = []
    for b in range(blocks):
        reads.append(pltpu.make_async_copy(w_ref.at[:, pl.ds(128 * b, 128), :], taken.at[b], in_sems.at[b]))
        reads[-1].start()
    lane = lax.broadcasted_iota(jnp.int32, (128, 128), 1)
    writes = []
    for b in range(blocks):
        reads[b].wait()
        for k, ((first, count), target) in enumerate(zip(parts(experts)[::2], swap_refs)):
            rows = taken.at[b, pl.ds(first, count), span(64 * away, 64), :]
            writes.append(
                pltpu.make_async_copy(rows, target.at[:, pl.ds(64 * b, 64), :], out_sems.at[2 * b + k])
            )
            writes[-1].start()
        total = jnp.zeros((128, 128), F32)
        for e in range(experts):
            row = jnp.max(jnp.abs(taken[b, e]), axis=1, keepdims=True)
            total = jnp.where(lane == e, row, total)
        out_ref[:, pl.ds(128 * b, 128)] = total.T[:experts]
    for write in writes:
        write.wait()


def local_maxima(f, w):
    experts, rows, _ = w.shape
    blocks = rows // 128
    return pl.pallas_call(
        local_kernel,
        out_shape=[
            array(experts, rows, kind=F32),
            *(array(count, rows // 2, 128, kind=F32) for _, count in parts(experts)[::2]),
        ],
        in_specs=[SMEM, ANY],
        out_specs=[VMEM, ANY, ANY],
        scratch_shapes=[
            pltpu.VMEM((blocks, experts, 128, 128), F32),
            pltpu.SemaphoreType.DMA((blocks,)),
            pltpu.SemaphoreType.DMA((2 * blocks,)),
        ],
        compiler_params=params(46),
        cost_estimate=cost(8 * 2**20, 4 * 2**20),
        name="local_maxima",
    )(f, w)


def swap_kernel(first, f_ref, w_ref, out_ref, taken, in_sems, out_sems):
    blocks, count = taken.shape[:2]
    away = 1 - f_ref[0] % 2
    reads, writes = [], []
    for b in range(blocks):
        rows = w_ref.at[pl.ds(first, count), span(128 * b + 64 * away, 64), :]
        reads.append(pltpu.make_async_copy(rows, taken.at[b], in_sems.at[b]))
        reads[-1].start()
    for b in range(blocks):
        reads[b].wait()
        writes.append(pltpu.make_async_copy(taken.at[b], out_ref.at[:, pl.ds(64 * b, 64), :], out_sems.at[b]))
        writes[-1].start()
    for write in writes:
        write.wait()


def swap_rows(f, w, first, count):
    rows = w.shape[1]
    blocks = rows // 128
    return pl.pallas_call(
        functools.partial(swap_kernel, first),
        out_shape=array(count, rows // 2, 128, kind=F32),
        in_specs=[SMEM, ANY],
        out_specs=ANY,
        scratch_shapes=[
            pltpu.VMEM((blocks, count, 64, 128), F32),
            pltpu.SemaphoreType.DMA((blocks,)),
            pltpu.SemaphoreType.DMA((blocks,)),
        ],
        compiler_params=params(46),
        cost_estimate=cost(3 * 2**20, 3 * 2**20),
        name="swap_rows",
    )(f, w)


def inverse_columns(scale_ref, inverse, slot, block):
    inverse[pl.ds(128 * slot, 128), :] = jnp.concatenate([1.0 / scale_ref[:, lanes(block)]] * 8, axis=0).T


def far_kernel(plan, f_ref, w_ref, theirs_ref, scale_ref, *refs):
    first, count, whole = plan
    outs, (taken, inverse, made, in_sems, out_sems) = refs[:-5], refs[-5:]
    f = f_ref[0]
    core = f % 2
    experts = pl.ds(first, count)
    reads = []
    for dx in range(4):
        q = 4 * (1 - f // 8) + dx if whole else chip(f, 1, dx)
        own = w_ref.at[experts, span(128 * q + 64 * core, 64), :]
        theirs = theirs_ref.at[:, span(64 * q, 64), :]
        for k, rows in enumerate((own, theirs)):
            reads.append(
                pltpu.make_async_copy(rows, taken.at[dx, pl.ds(k * count, count)], in_sems.at[2 * dx + k])
            )
            reads[-1].start()
    writes = []
    for dx in range(4):
        q = 4 * (1 - f // 8) + dx if whole else chip(f, 1, dx)
        inverse_columns(scale_ref, inverse, dx, q)
        columns = inverse[span(128 * dx + 64 * core, 64), :]
        for k in range(2):
            reads[2 * dx + k].wait()
            for e in range(count):
                at, lane = k * count + e, first + e
                made[dx, at] = (taken[dx, at] * columns[:, lane : lane + 1]).astype(BF16)
        target = outs[0].at[:, pl.ds(64 * dx, 64), :] if whole else outs[dx]
        writes.append(pltpu.make_async_copy(made.at[dx], target, out_sems.at[dx]))
        writes[-1].start()
    for write in writes:
        write.wait()


def far_pieces(f, w, theirs, scale, first, count, whole):
    outs = [array(2 * count, 256, 128)] if whole else [array(2 * count, 64, 128)] * 4
    return pl.pallas_call(
        functools.partial(far_kernel, (first, count, whole)),
        out_shape=outs,
        in_specs=[SMEM, ANY, ANY, VMEM],
        out_specs=[ANY] * len(outs),
        scratch_shapes=[
            pltpu.VMEM((4, 2 * count, 64, 128), F32),
            pltpu.VMEM((512, 128), F32),
            pltpu.VMEM((4, 2 * count, 64, 128), BF16),
            pltpu.SemaphoreType.DMA((8,)),
            pltpu.SemaphoreType.DMA((4,)),
        ],
        compiler_params=params(46),
        cost_estimate=cost(2 * 2**20, 2**20),
        name="far_pieces",
    )(f, w, theirs, scale)


def near_kernel(f_ref, w_ref, scale_ref, relay_ref, *refs):
    theirs_refs, outs, final_ref, refs = refs[:3], refs[3:6], refs[6], refs[7:]
    taken, relay, inverse, made, in_sems, out_sems = refs
    experts = w_ref.shape[0]
    late = experts - EARLY
    f = f_ref[0]
    core = f % 2
    reads = []
    for dx in range(4):
        q = chip(f, 0, dx)
        own = w_ref.at[:, span(128 * q + 64 * core, 64), :]
        rows = [(own, 0, experts)]
        for (first, count), theirs_ref in zip(parts(experts), theirs_refs):
            rows.append((theirs_ref.at[:, span(64 * q, 64), :], experts + first, count))
        for k, (piece, at, size) in enumerate(rows):
            reads.append(pltpu.make_async_copy(piece, taken.at[dx, pl.ds(at, size)], in_sems.at[4 * dx + k]))
            reads[-1].start()
    relayed = pltpu.make_async_copy(relay_ref, relay, in_sems.at[16])
    relayed.start()
    writes = []
    for dx in (1, 2, 3, 0):
        q = chip(f, 0, dx)
        inverse_columns(scale_ref, inverse, dx, q)
        columns = inverse[span(128 * dx + 64 * core, 64), :]
        for k in range(4):
            reads[4 * dx + k].wait()
        for k in range(2):
            for e in range(experts):
                at = k * experts + e
                made[dx, at] = (taken[dx, at] * columns[:, e : e + 1]).astype(BF16)
        if dx == 1:
            relayed.wait()
        for k in range(2):
            for j in range(EARLY):
                rows = relay[span(256 * (k * EARLY + j) + 64 * (q % 4), 64), :]
                lane = late + j
                made[dx, 2 * experts + k * EARLY + j] = (rows * columns[:, lane : lane + 1]).astype(BF16)
        if dx:
            copies = [pltpu.make_async_copy(made.at[dx], outs[dx - 1], out_sems.at[dx])]
        else:
            copies = near_copies(f, f // 2, made.at[0], final_ref, out_sems, 4)
        for copy in copies:
            copy.start()
        writes += copies
    for write in writes:
        write.wait()


def near_copies(f, source, piece, final_ref, sems, at):
    experts = final_ref.shape[0]
    across = (source + 4) % 8
    copies = []
    for k in range(2):
        side = f % 2 if k == 0 else 1 - f % 2
        copies.append((piece.at[pl.ds(k * experts, experts)], final_ref.at[:, :, lanes(2 * source + side)]))
        copies.append(
            (
                piece.at[pl.ds(2 * experts + k * EARLY, EARLY)],
                final_ref.at[pl.ds(experts - EARLY, EARLY), :, lanes(2 * across + side)],
            )
        )
    return [pltpu.make_async_copy(a, b, sems.at[at + k]) for k, (a, b) in enumerate(copies)]


def near_pieces(f, w, scale, relay, theirs):
    experts = w.shape[0]
    blocks = 2 * experts + 2 * EARLY
    return pl.pallas_call(
        near_kernel,
        out_shape=[array(blocks, 64, 128)] * 3 + [array(experts, 64, 2048)],
        in_specs=[SMEM, ANY, VMEM] + [ANY] * 4,
        out_specs=[ANY] * 4,
        scratch_shapes=[
            pltpu.VMEM((4, 2 * experts, 64, 128), F32),
            pltpu.VMEM(relay.shape, F32),
            pltpu.VMEM((512, 128), F32),
            pltpu.VMEM((4, blocks, 64, 128), BF16),
            pltpu.SemaphoreType.DMA((17,)),
            pltpu.SemaphoreType.DMA((8,)),
        ],
        compiler_params=params(46),
        cost_estimate=cost(5 * 2**20, 3 * 2**20),
        name="near_pieces",
    )(f, w, scale, relay, *theirs)


def split_kernel(f_ref, y_ref, chunk_ref, *refs):
    rows_refs, outs, final_ref, router_ref, made, sems = refs[:4], refs[5:8], refs[8], refs[9], refs[10], refs[11]
    f, y = f_ref[0], y_ref[0]
    count = chunk_ref.shape[0]
    copies = []
    for dx in (1, 2, 3):
        rows = chunk_ref.at[:, span(64 * (chip(f, 0, dx) % 4), 64), :]
        copies.append(pltpu.make_async_copy(rows, outs[dx - 1].at[pl.ds(0, count)], sems.at[dx]))
    rows = chunk_ref.at[:, span(64 * (chip(f, 0, 0) % 4), 64), :]
    copies += far_copies(f, chip(f, 1, 0), 0, rows, final_ref, sems, 4)
    for copy in copies:
        copy.start()
    for k in range(4):
        for dy, piece in enumerate(rows_refs):
            made[k, span((y - dy + 4) % 4 * 16, 16), :] = piece[k]
    more = [pltpu.make_async_copy(made, outs[dx - 1].at[pl.ds(count, 4)], sems.at[5 + dx]) for dx in (1, 2, 3)]
    run(more + router_copies(f, f // 2, made, router_ref, sems, 9))
    for copy in copies:
        copy.wait()


def router_copies(f, source, piece, router_ref, sems, at):
    copies = []
    for k in range(4):
        side = f % 2 if k < 2 else 1 - f % 2
        q = source if k % 2 == 0 else (source + 4) % 8
        copies.append(pltpu.make_async_copy(piece.at[k], router_ref.at[:, lanes(2 * q + side)], sems.at[at + k]))
    return copies


def far_copies(f, source, first, piece, final_ref, sems, at):
    count = piece.shape[0] // 2
    copies = []
    for k in range(2):
        side = f % 2 if k == 0 else 1 - f % 2
        target = final_ref.at[pl.ds(first, count), :, lanes(2 * source + side)]
        copies.append(pltpu.make_async_copy(piece.at[pl.ds(k * count, count)], target, sems.at[at + k]))
    return copies


def split(f, y, chunk, rows, final):
    count = chunk.shape[0]
    return pl.pallas_call(
        split_kernel,
        out_shape=[array(count + 4, 64, 128)] * 3 + [array(*final.shape), array(64, 2048)],
        in_specs=[SMEM, SMEM] + [VMEM] * 5 + [ANY],
        out_specs=[ANY] * 5,
        scratch_shapes=[pltpu.VMEM((4, 64, 128), BF16), pltpu.SemaphoreType.DMA((13,))],
        input_output_aliases={7: 3},
        compiler_params=params(46),
        cost_estimate=cost(2**20, 2**20),
        name="split",
    )(f, y, chunk, *rows, final)


def place_far_kernel(dx, first, f_ref, piece_ref, _, final_ref, sems):
    f = f_ref[0]
    run(far_copies(f, chip(f, 1, 4 - dx), first, piece_ref, final_ref, sems, 0))


def place_far(dx, first, f, piece, final):
    return pl.pallas_call(
        functools.partial(place_far_kernel, dx, first),
        out_shape=array(*final.shape),
        in_specs=[SMEM, VMEM, ANY],
        out_specs=ANY,
        scratch_shapes=[pltpu.SemaphoreType.DMA((2,))],
        input_output_aliases={2: 0},
        compiler_params=params(2),
        cost_estimate=cost(2**18, 2**18),
        name="place_far",
    )(f, piece, final)


def place_near_kernel(dx, f_ref, piece_ref, _, final_ref, sems):
    f = f_ref[0]
    run(near_copies(f, chip(f, 0, 4 - dx), piece_ref, final_ref, sems, 0))


def place_near(dx, f, piece, final):
    return pl.pallas_call(
        functools.partial(place_near_kernel, dx),
        out_shape=array(*final.shape),
        in_specs=[SMEM, VMEM, ANY],
        out_specs=ANY,
        scratch_shapes=[pltpu.SemaphoreType.DMA((4,))],
        input_output_aliases={2: 0},
        compiler_params=params(2),
        cost_estimate=cost(2**19, 2**19),
        name="place_near",
    )(f, piece, final)


def place_relayed_kernel(dx, f_ref, piece_ref, _, __, final_ref, router_ref, sems):
    f = f_ref[0]
    count = piece_ref.shape[0] - 4
    copies = far_copies(f, chip(f, 1, 4 - dx), 0, piece_ref.at[pl.ds(0, count)], final_ref, sems, 0)
    run(copies + router_copies(f, chip(f, 0, 4 - dx), piece_ref.at[pl.ds(count, 4)], router_ref, sems, 2))


def place_relayed(dx, f, piece, final, router):
    return pl.pallas_call(
        functools.partial(place_relayed_kernel, dx),
        out_shape=[array(*final.shape), array(*router.shape)],
        in_specs=[SMEM, VMEM, ANY, ANY],
        out_specs=[ANY, ANY],
        scratch_shapes=[pltpu.SemaphoreType.DMA((6,))],
        input_output_aliases={2: 0, 3: 1},
        compiler_params=params(2),
        cost_estimate=cost(2**18, 2**18),
        name="place_relayed",
    )(f, piece, final, router)


def served(w, router_weight, router_gain):
    experts, _, _ = w.shape
    position = lax.axis_index("fsdp")
    f = position.reshape(1)
    y = lax.axis_index("ep").reshape(1)
    far_plane = 1 - position // 8

    scale, swap, swap_early = local_maxima(f, w)
    theirs_early = send(swap_early, 0, 0, 1)
    peer = send(scale, 1, 0, 0)
    product = router_weight.T * router_gain.reshape(1, -1)
    own = lax.dynamic_slice(
        w.reshape(experts, 8, 2, 64, 128), (experts - EARLY, 4 * far_plane, position % 2, 0, 0), (EARLY, 4, 1, 64, 128)
    )
    other = lax.dynamic_slice(theirs_early, (0, 256 * far_plane, 0), (EARLY, 256, 128))
    early = jnp.concatenate([own.reshape(-1, 128), other.reshape(-1, 128), product])
    relay = send(early, 1, 0, 0)
    theirs = send(swap, 0, 0, 1)
    scale = jnp.maximum(scale, peer)
    scale = jnp.maximum(scale, send(scale, 0, 0, 1))
    scale = functools.reduce(jnp.maximum, [scale] + [send(scale, 0, dx, 0) for dx in (1, 3, 2)])
    direct = experts - RELAY - EARLY
    swap_direct = swap_rows(f, w, RELAY, direct)
    theirs_direct = send(swap_direct, 0, 0, 1)

    (chunk,) = far_pieces(f, w, theirs, scale, 0, RELAY, True)
    forward = send(chunk, 1, 0, 0)
    *pieces, final = near_pieces(f, w, scale, relay, (theirs, theirs_direct, theirs_early))
    plane = [send(piece, 0, k + 1, 0) for k, piece in enumerate(pieces)]
    pieces = far_pieces(f, w, theirs_direct, scale, RELAY, direct, False)
    across = [send(piece, 1, k, 0) for k, piece in enumerate(pieces)]
    near = jnp.stack([product, relay[2 * EARLY * 256 :]]).astype(BF16)
    near = jnp.concatenate([near, send(near, 0, 0, 1)])
    received = [near]
    for d in (1, 2, 3):
        received.append(lax.ppermute(near, "ep", [(i, (i + d) % 4) for i in range(4)]))
    *pieces, final, router = split(f, y, forward, received, final)
    relayed = [send(piece, 0, k + 1, 0) for k, piece in enumerate(pieces)]
    for k in range(3):
        final = place_near(k + 1, f, plane[k], final)
    for k in range(3):
        final, router = place_relayed(k + 1, f, relayed[k], final, router)
    for k in range(4):
        final = place_far(k, RELAY, f, across[k], final)
    own = lax.dynamic_slice_in_dim(scale, position * 64, 64, axis=1)
    return final, own, router.T


def solution(mesh):
    return jax.shard_map(
        served,
        mesh=mesh,
        in_specs=(
            P(("trial", "ep"), None, "fsdp"),
            P(("trial", "fsdp"), "ep"),
            P(("trial", "fsdp")),
        ),
        out_specs=(P(("trial", "ep"), "fsdp", None), P(("trial", "ep"), "fsdp"), P("trial", None)),
        check_vma=False,
    )
```

```python
import functools

import jax
import jax.numpy as jnp
from jax import lax
from jax.experimental import pallas as pl
from jax.experimental.pallas import tpu as pltpu
from jax.sharding import PartitionSpec as P


RELAY = 5
EARLY = 2
BF16, F32 = jnp.bfloat16, jnp.float32
ANY = pl.BlockSpec(memory_space=pl.ANY)
VMEM = pl.BlockSpec(memory_space=pltpu.VMEM)
SMEM = pl.BlockSpec(memory_space=pltpu.SMEM)


def params(mebibytes):
    return pltpu.CompilerParams(vmem_limit_bytes=mebibytes * 2**20)


def cost(read, written):
    return pl.CostEstimate(flops=(read + written) * 4, bytes_accessed=read + written, transcendentals=0)


def array(*shape, kind=BF16):
    return jax.ShapeDtypeStruct(shape, kind)


def span(start, size):
    return pl.ds(pl.multiple_of(start, size), size)


def lanes(position):
    return span(position * 128, 128)


def route(dz, dx, dc):
    pairs = []
    for f in range(16):
        z, x, c = f // 8, f // 2 % 4, f % 2
        pairs.append((f, (z ^ dz) * 8 + (x + dx) % 4 * 2 + (c ^ dc)))
    return pairs


def send(piece, dz, dx, dc):
    return lax.ppermute(piece, "fsdp", route(dz, dx, dc))


def chip(f, dz, dx):
    z = f // 8 if dz == 0 else 1 - f // 8
    return z * 4 + (f // 2 + dx) % 4


def run(copies):
    for copy in copies:
        copy.start()
    for copy in copies:
        copy.wait()


def local_kernel(f_ref, w_ref, mine_ref, theirs_ref, swap_ref, taken, in_sems, out_sems):
    blocks, experts = taken.shape[:2]
    core = f_ref[0] % 2
    reads = []
    for b in range(blocks):
        reads.append(pltpu.make_async_copy(w_ref.at[:, pl.ds(128 * b, 128), :], taken.at[b], in_sems.at[b]))
        reads[-1].start()
    lane = lax.broadcasted_iota(jnp.int32, (128, 128), 1)
    low = lax.broadcasted_iota(jnp.int32, (experts, 128), 1) < 64
    writes, rows = [], []
    for b in range(blocks):
        reads[b].wait()
        piece = taken.at[b, pl.ds(0, RELAY), span(64 * (1 - core), 64), :]
        writes.append(pltpu.make_async_copy(piece, swap_ref.at[:, pl.ds(64 * b, 64), :], out_sems.at[b]))
        writes[-1].start()
        total = jnp.zeros((128, 128), F32)
        for e in range(experts):
            row = jnp.max(jnp.abs(taken[b, e]), axis=1, keepdims=True)
            total = jnp.where(lane == e, row, total)
        rows.append(total.T[:experts])
        if b % 2:
            first, second = rows[-2:]
            south = jnp.where(low, first, pltpu.roll(second, 64, 1))
            north = jnp.where(low, pltpu.roll(first, 64, 1), second)
            at = pl.ds(64 * (b - 1), 128)
            mine_ref[:, at] = jnp.where(core == 0, south, north)
            theirs_ref[:, at] = jnp.where(core == 0, north, south)
    for write in writes:
        write.wait()


def local_maxima(f, w):
    experts, rows, _ = w.shape
    blocks = rows // 128
    return pl.pallas_call(
        local_kernel,
        out_shape=[
            array(experts, rows // 2, kind=F32),
            array(experts, rows // 2, kind=F32),
            array(RELAY, rows // 2, 128, kind=F32),
        ],
        in_specs=[SMEM, ANY],
        out_specs=[VMEM, VMEM, ANY],
        scratch_shapes=[
            pltpu.VMEM((blocks, experts, 128, 128), F32),
            pltpu.SemaphoreType.DMA((blocks,)),
            pltpu.SemaphoreType.DMA((blocks,)),
        ],
        compiler_params=params(46),
        cost_estimate=cost(8 * 2**20, 4 * 2**20),
        name="local_maxima",
    )(f, w)


def swap_kernel(first, f_ref, w_ref, out_ref, taken, in_sems, out_sems):
    blocks, count = taken.shape[:2]
    away = 1 - f_ref[0] % 2
    reads, writes = [], []
    for b in range(blocks):
        rows = w_ref.at[pl.ds(first, count), span(128 * b + 64 * away, 64), :]
        reads.append(pltpu.make_async_copy(rows, taken.at[b], in_sems.at[b]))
        reads[-1].start()
    for b in range(blocks):
        reads[b].wait()
        writes.append(pltpu.make_async_copy(taken.at[b], out_ref.at[:, pl.ds(64 * b, 64), :], out_sems.at[b]))
        writes[-1].start()
    for write in writes:
        write.wait()


def swap_rows(f, w, first, count):
    rows = w.shape[1]
    blocks = rows // 128
    return pl.pallas_call(
        functools.partial(swap_kernel, first),
        out_shape=array(count, rows // 2, 128, kind=F32),
        in_specs=[SMEM, ANY],
        out_specs=ANY,
        scratch_shapes=[
            pltpu.VMEM((blocks, count, 64, 128), F32),
            pltpu.SemaphoreType.DMA((blocks,)),
            pltpu.SemaphoreType.DMA((blocks,)),
        ],
        compiler_params=params(46),
        cost_estimate=cost(3 * 2**20, 3 * 2**20),
        name="swap_rows",
    )(f, w)


def inverse_columns(scale_ref, inverse):
    for b in range(4):
        block = 1.0 / scale_ref[:, pl.ds(128 * b, 128)]
        inverse[pl.ds(128 * b, 128), :] = jnp.concatenate([block] * 8, axis=0).T


def far_kernel(plan, f_ref, w_ref, theirs_ref, scale_ref, *refs):
    first, count, whole = plan
    outs, (taken, inverse, made, in_sems, out_sems) = refs[:-5], refs[-5:]
    f = f_ref[0]
    core = f % 2
    experts = pl.ds(first, count)
    reads = []
    for dx in range(4):
        q = 4 * (1 - f // 8) + dx if whole else chip(f, 1, dx)
        own = w_ref.at[experts, span(128 * q + 64 * core, 64), :]
        theirs = theirs_ref.at[pl.ds(0, count), span(64 * q, 64), :]
        for k, rows in enumerate((own, theirs)):
            reads.append(
                pltpu.make_async_copy(rows, taken.at[dx, pl.ds(k * count, count)], in_sems.at[2 * dx + k])
            )
            reads[-1].start()
    inverse_columns(scale_ref, inverse)
    writes = []
    for dx in range(4):
        q = 4 * (1 - f // 8) + dx if whole else chip(f, 1, dx)
        columns = inverse[span(64 * q, 64), :]
        for k in range(2):
            reads[2 * dx + k].wait()
            for e in range(count):
                at, lane = k * count + e, first + e
                made[dx, at] = (taken[dx, at] * columns[:, lane : lane + 1]).astype(BF16)
        target = outs[0].at[:, pl.ds(64 * dx, 64), :] if whole else outs[dx]
        writes.append(pltpu.make_async_copy(made.at[dx], target, out_sems.at[dx]))
        writes[-1].start()
    for write in writes:
        write.wait()


def far_pieces(f, w, theirs, scale, first, count, whole):
    outs = [array(2 * count, 256, 128)] if whole else [array(2 * count, 64, 128)] * 4
    return pl.pallas_call(
        functools.partial(far_kernel, (first, count, whole)),
        out_shape=outs,
        in_specs=[SMEM, ANY, ANY, VMEM],
        out_specs=[ANY] * len(outs),
        scratch_shapes=[
            pltpu.VMEM((4, 2 * count, 64, 128), F32),
            pltpu.VMEM((512, 128), F32),
            pltpu.VMEM((4, 2 * count, 64, 128), BF16),
            pltpu.SemaphoreType.DMA((8,)),
            pltpu.SemaphoreType.DMA((4,)),
        ],
        compiler_params=params(46),
        cost_estimate=cost(2 * 2**20, 2**20),
        name="far_pieces",
    )(f, w, theirs, scale)


def near_kernel(f_ref, w_ref, scale_ref, *refs):
    early_refs, (across_ref, theirs_ref, rest_ref), refs = refs[:EARLY], refs[EARLY : EARLY + 3], refs[EARLY + 3 :]
    outs, final_ref, (taken, relay, inverse, made, in_sems, out_sems) = refs[:3], refs[3], refs[4:]
    experts = w_ref.shape[0]
    late = experts - EARLY
    f = f_ref[0]
    core = f % 2
    reads = []
    for dx in range(4):
        q = chip(f, 0, dx)
        for k, (piece, at, size) in enumerate(
            (
                (w_ref.at[:, span(128 * q + 64 * core, 64), :], 0, experts),
                (theirs_ref.at[:, span(64 * q, 64), :], experts, RELAY),
                (rest_ref.at[:, span(64 * q, 64), :], experts + RELAY, experts - RELAY),
            )
        ):
            reads.append(pltpu.make_async_copy(piece, taken.at[dx, pl.ds(at, size)], in_sems.at[3 * dx + k]))
            reads[-1].start()
    half = 256 * EARLY
    relayed = [pltpu.make_async_copy(across_ref, relay.at[pl.ds(half, half)], in_sems.at[12])]
    for j, early_ref in enumerate(early_refs):
        for k in range(4):
            rows = early_ref.at[span(128 * k + 64 * core, 64), :]
            target = relay.at[pl.ds(256 * j + 64 * k, 64)]
            relayed.append(pltpu.make_async_copy(rows, target, in_sems.at[13 + 4 * j + k]))
    for copy in relayed:
        copy.start()
    inverse_columns(scale_ref, inverse)
    writes = []
    for dx in (1, 2, 3, 0):
        q = chip(f, 0, dx)
        columns = inverse[span(64 * q, 64), :]
        for k in range(3):
            reads[3 * dx + k].wait()
        for k in range(2):
            for e in range(experts):
                at = k * experts + e
                made[dx, at] = (taken[dx, at] * columns[:, e : e + 1]).astype(BF16)
        if dx == 1:
            for copy in relayed:
                copy.wait()
        for k in range(2):
            for j in range(EARLY):
                rows = relay[span(256 * (k * EARLY + j) + 64 * (q % 4), 64), :]
                lane = late + j
                made[dx, 2 * experts + k * EARLY + j] = (rows * columns[:, lane : lane + 1]).astype(BF16)
        if dx:
            copies = [pltpu.make_async_copy(made.at[dx], outs[dx - 1], out_sems.at[dx])]
        else:
            copies = near_copies(f, f // 2, made.at[0], final_ref, out_sems, 4)
        for copy in copies:
            copy.start()
        writes += copies
    for write in writes:
        write.wait()


def near_copies(f, source, piece, final_ref, sems, at):
    experts = final_ref.shape[0]
    across = (source + 4) % 8
    copies = []
    for k in range(2):
        side = f % 2 if k == 0 else 1 - f % 2
        copies.append((piece.at[pl.ds(k * experts, experts)], final_ref.at[:, :, lanes(2 * source + side)]))
        copies.append(
            (
                piece.at[pl.ds(2 * experts + k * EARLY, EARLY)],
                final_ref.at[pl.ds(experts - EARLY, EARLY), :, lanes(2 * across + side)],
            )
        )
    return [pltpu.make_async_copy(a, b, sems.at[at + k]) for k, (a, b) in enumerate(copies)]


def near_pieces(f, w, scale, early, across, theirs, rest):
    experts = w.shape[0]
    blocks = 2 * experts + 2 * EARLY
    return pl.pallas_call(
        near_kernel,
        out_shape=[array(blocks, 64, 128)] * 3 + [array(experts, 64, 2048)],
        in_specs=[SMEM, ANY, VMEM] + [ANY] * (EARLY + 3),
        out_specs=[ANY] * 4,
        scratch_shapes=[
            pltpu.VMEM((4, 2 * experts, 64, 128), F32),
            pltpu.VMEM((512 * EARLY, 128), F32),
            pltpu.VMEM((512, 128), F32),
            pltpu.VMEM((4, blocks, 64, 128), BF16),
            pltpu.SemaphoreType.DMA((13 + 4 * EARLY,)),
            pltpu.SemaphoreType.DMA((8,)),
        ],
        compiler_params=params(46),
        cost_estimate=cost(5 * 2**20, 3 * 2**20),
        name="near_pieces",
    )(f, w, scale, *early, across, theirs, rest)


def split_kernel(f_ref, y_ref, chunk_ref, *refs):
    rows_refs, outs, final_ref, router_ref, made, sems = refs[:4], refs[5:8], refs[8], refs[9], refs[10], refs[11]
    f, y = f_ref[0], y_ref[0]
    count = chunk_ref.shape[0]
    copies = []
    for dx in (1, 2, 3):
        rows = chunk_ref.at[:, span(64 * (chip(f, 0, dx) % 4), 64), :]
        copies.append(pltpu.make_async_copy(rows, outs[dx - 1].at[pl.ds(0, count)], sems.at[dx]))
    rows = chunk_ref.at[:, span(64 * (chip(f, 0, 0) % 4), 64), :]
    copies += far_copies(f, chip(f, 1, 0), 0, rows, final_ref, sems, 4)
    for copy in copies:
        copy.start()
    for k in range(4):
        for dy, piece in enumerate(rows_refs):
            made[k, span((y - dy + 4) % 4 * 16, 16), :] = piece[k]
    more = [pltpu.make_async_copy(made, outs[dx - 1].at[pl.ds(count, 4)], sems.at[5 + dx]) for dx in (1, 2, 3)]
    run(more + router_copies(f, f // 2, made, router_ref, sems, 9))
    for copy in copies:
        copy.wait()


def router_copies(f, source, piece, router_ref, sems, at):
    copies = []
    for k in range(4):
        side = f % 2 if k < 2 else 1 - f % 2
        q = source if k % 2 == 0 else (source + 4) % 8
        copies.append(pltpu.make_async_copy(piece.at[k], router_ref.at[:, lanes(2 * q + side)], sems.at[at + k]))
    return copies


def far_copies(f, source, first, piece, final_ref, sems, at):
    count = piece.shape[0] // 2
    copies = []
    for k in range(2):
        side = f % 2 if k == 0 else 1 - f % 2
        target = final_ref.at[pl.ds(first, count), :, lanes(2 * source + side)]
        copies.append(pltpu.make_async_copy(piece.at[pl.ds(k * count, count)], target, sems.at[at + k]))
    return copies


def split(f, y, chunk, rows, final):
    count = chunk.shape[0]
    return pl.pallas_call(
        split_kernel,
        out_shape=[array(count + 4, 64, 128)] * 3 + [array(*final.shape), array(64, 2048)],
        in_specs=[SMEM, SMEM] + [VMEM] * 5 + [ANY],
        out_specs=[ANY] * 5,
        scratch_shapes=[pltpu.VMEM((4, 64, 128), BF16), pltpu.SemaphoreType.DMA((13,))],
        input_output_aliases={7: 3},
        compiler_params=params(46),
        cost_estimate=cost(2**20, 2**20),
        name="split",
    )(f, y, chunk, *rows, final)


def place_far_kernel(dx, first, f_ref, piece_ref, _, final_ref, sems):
    f = f_ref[0]
    run(far_copies(f, chip(f, 1, 4 - dx), first, piece_ref, final_ref, sems, 0))


def place_far(dx, first, f, piece, final):
    return pl.pallas_call(
        functools.partial(place_far_kernel, dx, first),
        out_shape=array(*final.shape),
        in_specs=[SMEM, VMEM, ANY],
        out_specs=ANY,
        scratch_shapes=[pltpu.SemaphoreType.DMA((2,))],
        input_output_aliases={2: 0},
        compiler_params=params(2),
        cost_estimate=cost(2**18, 2**18),
        name="place_far",
    )(f, piece, final)


def place_near_kernel(dx, f_ref, piece_ref, _, final_ref, sems):
    f = f_ref[0]
    run(near_copies(f, chip(f, 0, 4 - dx), piece_ref, final_ref, sems, 0))


def place_near(dx, f, piece, final):
    return pl.pallas_call(
        functools.partial(place_near_kernel, dx),
        out_shape=array(*final.shape),
        in_specs=[SMEM, VMEM, ANY],
        out_specs=ANY,
        scratch_shapes=[pltpu.SemaphoreType.DMA((4,))],
        input_output_aliases={2: 0},
        compiler_params=params(2),
        cost_estimate=cost(2**19, 2**19),
        name="place_near",
    )(f, piece, final)


def place_relayed_kernel(dx, f_ref, piece_ref, _, __, final_ref, router_ref, sems):
    f = f_ref[0]
    count = piece_ref.shape[0] - 4
    copies = far_copies(f, chip(f, 1, 4 - dx), 0, piece_ref.at[pl.ds(0, count)], final_ref, sems, 0)
    run(copies + router_copies(f, chip(f, 0, 4 - dx), piece_ref.at[pl.ds(count, 4)], router_ref, sems, 2))


def place_relayed(dx, f, piece, final, router):
    return pl.pallas_call(
        functools.partial(place_relayed_kernel, dx),
        out_shape=[array(*final.shape), array(*router.shape)],
        in_specs=[SMEM, VMEM, ANY, ANY],
        out_specs=[ANY, ANY],
        scratch_shapes=[pltpu.SemaphoreType.DMA((6,))],
        input_output_aliases={2: 0, 3: 1},
        compiler_params=params(2),
        cost_estimate=cost(2**18, 2**18),
        name="place_relayed",
    )(f, piece, final, router)


def served(w, router_weight, router_gain):
    experts, _, _ = w.shape
    late, direct = experts - EARLY, experts - RELAY - EARLY
    position = lax.axis_index("fsdp")
    f = position.reshape(1)
    y = lax.axis_index("ep").reshape(1)
    far_plane, core = 1 - position // 8, position % 2

    soon = lax.dynamic_slice(w, (experts - 1, 512 * far_plane, 0), (1, 512, 128)).reshape(512, 128)
    soon = send(soon, 1, 0, 0)
    scale, scale_theirs, swap = local_maxima(f, w)
    scale = jnp.maximum(scale, send(scale_theirs, 0, 0, 1))
    peer = send(scale, 1, 0, 0)
    product = router_weight.T * router_gain.reshape(1, -1)
    early = lax.dynamic_slice(w, (late, 512 * far_plane, 0), (EARLY - 1, 512, 128))
    early = jnp.concatenate([early.reshape(-1, 128), product])
    early = send(early, 1, 0, 0)
    theirs = send(swap, 0, 0, 1)
    scale = jnp.maximum(scale, peer)
    scale = functools.reduce(jnp.maximum, [scale] + [send(scale, 0, dx, 0) for dx in (1, 3, 2)])
    swap_rest = swap_rows(f, w, RELAY, experts - RELAY)
    rest = send(swap_rest, 0, 0, 1)

    (chunk,) = far_pieces(f, w, theirs, scale, 0, RELAY, True)
    forward = send(chunk, 1, 0, 0)
    relay = [early[512 * j : 512 * (j + 1)] for j in range(EARLY - 1)] + [soon]
    turned = jnp.stack(relay).reshape(EARLY, 4, 2, 64, 128)
    turned = lax.dynamic_slice_in_dim(turned, 1 - core, 1, axis=2).reshape(EARLY * 256, 128)
    turned = send(turned, 0, 0, 1)
    *pieces, final = near_pieces(f, w, scale, [early] + [soon], turned, theirs, rest)
    plane = [send(piece, 0, k + 1, 0) for k, piece in enumerate(pieces)]
    pieces = far_pieces(f, w, rest, scale, RELAY, direct, False)
    across = [send(piece, 1, k, 0) for k, piece in enumerate(pieces)]
    near = jnp.stack([product, early[-16:]]).astype(BF16)
    near = jnp.concatenate([near, send(near, 0, 0, 1)])
    received = [near]
    for d in (1, 2, 3):
        received.append(lax.ppermute(near, "ep", [(i, (i + d) % 4) for i in range(4)]))
    *pieces, final, router = split(f, y, forward, received, final)
    relayed = [send(piece, 0, k + 1, 0) for k, piece in enumerate(pieces)]
    for k in range(3):
        final = place_near(k + 1, f, plane[k], final)
    for k in range(3):
        final, router = place_relayed(k + 1, f, relayed[k], final, router)
    for k in range(4):
        final = place_far(k, RELAY, f, across[k], final)
    own = lax.dynamic_slice_in_dim(scale, position // 2 * 64, 64, axis=1)
    return final, own, router.T


def solution(mesh):
    return jax.shard_map(
        served,
        mesh=mesh,
        in_specs=(
            P(("trial", "ep"), None, "fsdp"),
            P(("trial", "fsdp"), "ep"),
            P(("trial", "fsdp")),
        ),
        out_specs=(P(("trial", "ep"), "fsdp", None), P(("trial", "ep"), "fsdp"), P("trial", None)),
        check_vma=False,
    )
```

```python
import functools

import jax
import jax.numpy as jnp
from jax import lax
from jax.experimental import pallas as pl
from jax.experimental.pallas import tpu as pltpu
from jax.sharding import PartitionSpec as P


RELAY = 3
EARLY = 1
BF16, F32 = jnp.bfloat16, jnp.float32
ANY = pl.BlockSpec(memory_space=pl.ANY)
VMEM = pl.BlockSpec(memory_space=pltpu.VMEM)
SMEM = pl.BlockSpec(memory_space=pltpu.SMEM)


def params(mebibytes):
    return pltpu.CompilerParams(vmem_limit_bytes=mebibytes * 2**20)


def cost(read, written):
    return pl.CostEstimate(flops=(read + written) * 4, bytes_accessed=read + written, transcendentals=0)


def array(*shape, kind=BF16):
    return jax.ShapeDtypeStruct(shape, kind)


def span(start, size):
    return pl.ds(pl.multiple_of(start, size), size)


def lanes(position):
    return span(position * 128, 128)


def route(dz, dx, dc):
    pairs = []
    for f in range(16):
        z, x, c = f // 8, f // 2 % 4, f % 2
        pairs.append((f, (z ^ dz) * 8 + (x + dx) % 4 * 2 + (c ^ dc)))
    return pairs


def send(piece, dz, dx, dc):
    return lax.ppermute(piece, "fsdp", route(dz, dx, dc))


def chip(f, dz, dx):
    z = f // 8 if dz == 0 else 1 - f // 8
    return z * 4 + (f // 2 + dx) % 4


def run(copies):
    for copy in copies:
        copy.start()
    for copy in copies:
        copy.wait()


def local_kernel(f_ref, w_ref, mine_ref, theirs_ref, swap_ref, rest_ref, taken, in_sems, out_sems):
    blocks, experts = taken.shape[:2]
    core = f_ref[0] % 2
    reads = []
    for b in range(blocks):
        reads.append(pltpu.make_async_copy(w_ref.at[:, pl.ds(128 * b, 128), :], taken.at[b], in_sems.at[b]))
        reads[-1].start()
    lane = lax.broadcasted_iota(jnp.int32, (128, 128), 1)
    low = lax.broadcasted_iota(jnp.int32, (experts, 128), 1) < 64
    writes, rows = [], []
    for b in range(blocks):
        reads[b].wait()
        for k, (first, target) in enumerate(((0, swap_ref), (RELAY, rest_ref))):
            piece = taken.at[b, pl.ds(first, target.shape[0]), span(64 * (1 - core), 64), :]
            target = target.at[:, pl.ds(64 * b, 64), :]
            writes.append(pltpu.make_async_copy(piece, target, out_sems.at[2 * b + k]))
            writes[-1].start()
        total = jnp.zeros((128, 128), F32)
        for e in range(experts):
            row = jnp.max(jnp.abs(taken[b, e]), axis=1, keepdims=True)
            total = jnp.where(lane == e, row, total)
        rows.append(total.T[:experts])
        if b % 2:
            first, second = rows[-2:]
            south = jnp.where(low, first, pltpu.roll(second, 64, 1))
            north = jnp.where(low, pltpu.roll(first, 64, 1), second)
            at = pl.ds(64 * (b - 1), 128)
            mine_ref[:, at] = jnp.where(core == 0, south, north)
            theirs_ref[:, at] = jnp.where(core == 0, north, south)
    for write in writes:
        write.wait()


def local_maxima(f, w):
    experts, rows, _ = w.shape
    blocks = rows // 128
    return pl.pallas_call(
        local_kernel,
        out_shape=[
            array(experts, rows // 2, kind=F32),
            array(experts, rows // 2, kind=F32),
            array(RELAY, rows // 2, 128, kind=F32),
            array(experts - RELAY, rows // 2, 128, kind=F32),
        ],
        in_specs=[SMEM, ANY],
        out_specs=[VMEM, VMEM, ANY, ANY],
        scratch_shapes=[
            pltpu.VMEM((blocks, experts, 128, 128), F32),
            pltpu.SemaphoreType.DMA((blocks,)),
            pltpu.SemaphoreType.DMA((2 * blocks,)),
        ],
        compiler_params=params(50),
        cost_estimate=cost(8 * 2**20, 4 * 2**20),
        name="local_maxima",
    )(f, w)


def inverse_columns(scale_ref, inverse):
    for b in range(4):
        block = 1.0 / scale_ref[:, pl.ds(128 * b, 128)]
        inverse[pl.ds(128 * b, 128), :] = jnp.concatenate([block] * 8, axis=0).T


def far_kernel(plan, f_ref, w_ref, theirs_ref, scale_ref, *refs):
    first, count, whole = plan
    outs, (taken, inverse, made, in_sems, out_sems) = refs[:-5], refs[-5:]
    f = f_ref[0]
    core = f % 2
    experts = pl.ds(first, count)
    reads = []
    for dx in range(4):
        q = 4 * (1 - f // 8) + dx if whole else chip(f, 1, dx)
        own = w_ref.at[experts, span(128 * q + 64 * core, 64), :]
        theirs = theirs_ref.at[pl.ds(0, count), span(64 * q, 64), :]
        for k, rows in enumerate((own, theirs)):
            reads.append(
                pltpu.make_async_copy(rows, taken.at[dx, pl.ds(k * count, count)], in_sems.at[2 * dx + k])
            )
            reads[-1].start()
    inverse_columns(scale_ref, inverse)
    writes = []
    for dx in range(4):
        q = 4 * (1 - f // 8) + dx if whole else chip(f, 1, dx)
        columns = inverse[span(64 * q, 64), :]
        for k in range(2):
            reads[2 * dx + k].wait()
            for e in range(count):
                at, lane = k * count + e, first + e
                made[dx, at] = (taken[dx, at] * columns[:, lane : lane + 1]).astype(BF16)
        target = outs[0].at[:, pl.ds(64 * dx, 64), :] if whole else outs[dx]
        writes.append(pltpu.make_async_copy(made.at[dx], target, out_sems.at[dx]))
        writes[-1].start()
    for write in writes:
        write.wait()


def far_pieces(f, w, theirs, scale, first, count, whole):
    outs = [array(2 * count, 256, 128)] if whole else [array(2 * count, 64, 128)] * 4
    return pl.pallas_call(
        functools.partial(far_kernel, (first, count, whole)),
        out_shape=outs,
        in_specs=[SMEM, ANY, ANY, VMEM],
        out_specs=[ANY] * len(outs),
        scratch_shapes=[
            pltpu.VMEM((4, 2 * count, 64, 128), F32),
            pltpu.VMEM((512, 128), F32),
            pltpu.VMEM((4, 2 * count, 64, 128), BF16),
            pltpu.SemaphoreType.DMA((8,)),
            pltpu.SemaphoreType.DMA((4,)),
        ],
        compiler_params=params(50),
        cost_estimate=cost(2 * 2**20, 2**20),
        name="far_pieces",
    )(f, w, theirs, scale)


def near_kernel(f_ref, w_ref, scale_ref, *refs):
    (early_ref, across_ref, theirs_ref, rest_ref), refs = refs[:4], refs[4:]
    outs, final_ref, (taken, relay, inverse, made, in_sems, out_sems) = refs[:3], refs[3], refs[4:]
    experts = w_ref.shape[0]
    late = experts - EARLY
    f = f_ref[0]
    core = f % 2
    reads = []
    for dx in range(4):
        q = chip(f, 0, dx)
        for k, (piece, at, size) in enumerate(
            (
                (w_ref.at[:, span(128 * q + 64 * core, 64), :], 0, experts),
                (theirs_ref.at[:, span(64 * q, 64), :], experts, RELAY),
                (rest_ref.at[:, span(64 * q, 64), :], experts + RELAY, experts - RELAY),
            )
        ):
            reads.append(pltpu.make_async_copy(piece, taken.at[dx, pl.ds(at, size)], in_sems.at[3 * dx + k]))
            reads[-1].start()
    half = 256 * EARLY
    relayed = [pltpu.make_async_copy(across_ref, relay.at[pl.ds(half, half)], in_sems.at[12])]
    for k in range(4 * EARLY):
        rows = early_ref.at[span(128 * k + 64 * core, 64), :]
        relayed.append(pltpu.make_async_copy(rows, relay.at[pl.ds(64 * k, 64)], in_sems.at[13 + k]))
    for copy in relayed:
        copy.start()
    inverse_columns(scale_ref, inverse)
    writes = []
    for dx in (1, 2, 3, 0):
        q = chip(f, 0, dx)
        columns = inverse[span(64 * q, 64), :]
        for k in range(3):
            reads[3 * dx + k].wait()
        for k in range(2):
            for e in range(experts):
                at = k * experts + e
                made[dx, at] = (taken[dx, at] * columns[:, e : e + 1]).astype(BF16)
        if dx == 1:
            for copy in relayed:
                copy.wait()
        for k in range(2):
            for j in range(EARLY):
                rows = relay[span(256 * (k * EARLY + j) + 64 * (q % 4), 64), :]
                lane = late + j
                made[dx, 2 * experts + k * EARLY + j] = (rows * columns[:, lane : lane + 1]).astype(BF16)
        if dx:
            copies = [pltpu.make_async_copy(made.at[dx], outs[dx - 1], out_sems.at[dx])]
        else:
            copies = near_copies(f, f // 2, made.at[0], final_ref, out_sems, 4)
        for copy in copies:
            copy.start()
        writes += copies
    for write in writes:
        write.wait()


def near_copies(f, source, piece, final_ref, sems, at):
    experts = final_ref.shape[0]
    across = (source + 4) % 8
    copies = []
    for k in range(2):
        side = f % 2 if k == 0 else 1 - f % 2
        copies.append((piece.at[pl.ds(k * experts, experts)], final_ref.at[:, :, lanes(2 * source + side)]))
        copies.append(
            (
                piece.at[pl.ds(2 * experts + k * EARLY, EARLY)],
                final_ref.at[pl.ds(experts - EARLY, EARLY), :, lanes(2 * across + side)],
            )
        )
    return [pltpu.make_async_copy(a, b, sems.at[at + k]) for k, (a, b) in enumerate(copies)]


def near_pieces(f, w, scale, early, across, theirs, rest):
    experts = w.shape[0]
    blocks = 2 * experts + 2 * EARLY
    return pl.pallas_call(
        near_kernel,
        out_shape=[array(blocks, 64, 128)] * 3 + [array(experts, 64, 2048)],
        in_specs=[SMEM, ANY, VMEM] + [ANY] * 4,
        out_specs=[ANY] * 4,
        scratch_shapes=[
            pltpu.VMEM((4, 2 * experts, 64, 128), F32),
            pltpu.VMEM((512 * EARLY, 128), F32),
            pltpu.VMEM((512, 128), F32),
            pltpu.VMEM((4, blocks, 64, 128), BF16),
            pltpu.SemaphoreType.DMA((13 + 4 * EARLY,)),
            pltpu.SemaphoreType.DMA((8,)),
        ],
        compiler_params=params(50),
        cost_estimate=cost(5 * 2**20, 3 * 2**20),
        name="near_pieces",
    )(f, w, scale, early, across, theirs, rest)


def split_kernel(f_ref, y_ref, chunk_ref, *refs):
    rows_refs, outs, final_ref, router_ref, made, sems = refs[:4], refs[5:8], refs[8], refs[9], refs[10], refs[11]
    f, y = f_ref[0], y_ref[0]
    count = chunk_ref.shape[0]
    copies = []
    for dx in (1, 2, 3):
        rows = chunk_ref.at[:, span(64 * (chip(f, 0, dx) % 4), 64), :]
        copies.append(pltpu.make_async_copy(rows, outs[dx - 1].at[pl.ds(0, count)], sems.at[dx]))
    rows = chunk_ref.at[:, span(64 * (chip(f, 0, 0) % 4), 64), :]
    copies += far_copies(f, chip(f, 1, 0), 0, rows, final_ref, sems, 4)
    for copy in copies:
        copy.start()
    for k in range(4):
        for dy, piece in enumerate(rows_refs):
            made[k, span((y - dy + 4) % 4 * 16, 16), :] = piece[k]
    more = [pltpu.make_async_copy(made, outs[dx - 1].at[pl.ds(count, 4)], sems.at[5 + dx]) for dx in (1, 2, 3)]
    run(more + router_copies(f, f // 2, made, router_ref, sems, 9))
    for copy in copies:
        copy.wait()


def router_copies(f, source, piece, router_ref, sems, at):
    copies = []
    for k in range(4):
        side = f % 2 if k < 2 else 1 - f % 2
        q = source if k % 2 == 0 else (source + 4) % 8
        copies.append(pltpu.make_async_copy(piece.at[k], router_ref.at[:, lanes(2 * q + side)], sems.at[at + k]))
    return copies


def far_copies(f, source, first, piece, final_ref, sems, at):
    count = piece.shape[0] // 2
    copies = []
    for k in range(2):
        side = f % 2 if k == 0 else 1 - f % 2
        target = final_ref.at[pl.ds(first, count), :, lanes(2 * source + side)]
        copies.append(pltpu.make_async_copy(piece.at[pl.ds(k * count, count)], target, sems.at[at + k]))
    return copies


def split(f, y, chunk, rows, final):
    count = chunk.shape[0]
    return pl.pallas_call(
        split_kernel,
        out_shape=[array(count + 4, 64, 128)] * 3 + [array(*final.shape), array(64, 2048)],
        in_specs=[SMEM, SMEM] + [VMEM] * 5 + [ANY],
        out_specs=[ANY] * 5,
        scratch_shapes=[pltpu.VMEM((4, 64, 128), BF16), pltpu.SemaphoreType.DMA((13,))],
        input_output_aliases={7: 3},
        compiler_params=params(50),
        cost_estimate=cost(2**20, 2**20),
        name="split",
    )(f, y, chunk, *rows, final)


def place_far_kernel(dx, first, f_ref, piece_ref, _, final_ref, sems):
    f = f_ref[0]
    run(far_copies(f, chip(f, 1, 4 - dx), first, piece_ref, final_ref, sems, 0))


def place_far(dx, first, f, piece, final):
    return pl.pallas_call(
        functools.partial(place_far_kernel, dx, first),
        out_shape=array(*final.shape),
        in_specs=[SMEM, VMEM, ANY],
        out_specs=ANY,
        scratch_shapes=[pltpu.SemaphoreType.DMA((2,))],
        input_output_aliases={2: 0},
        compiler_params=params(2),
        cost_estimate=cost(2**18, 2**18),
        name="place_far",
    )(f, piece, final)


def place_near_kernel(dx, f_ref, piece_ref, _, final_ref, sems):
    f = f_ref[0]
    run(near_copies(f, chip(f, 0, 4 - dx), piece_ref, final_ref, sems, 0))


def place_near(dx, f, piece, final):
    return pl.pallas_call(
        functools.partial(place_near_kernel, dx),
        out_shape=array(*final.shape),
        in_specs=[SMEM, VMEM, ANY],
        out_specs=ANY,
        scratch_shapes=[pltpu.SemaphoreType.DMA((4,))],
        input_output_aliases={2: 0},
        compiler_params=params(2),
        cost_estimate=cost(2**19, 2**19),
        name="place_near",
    )(f, piece, final)


def place_relayed_kernel(dx, f_ref, piece_ref, _, __, final_ref, router_ref, sems):
    f = f_ref[0]
    count = piece_ref.shape[0] - 4
    copies = far_copies(f, chip(f, 1, 4 - dx), 0, piece_ref.at[pl.ds(0, count)], final_ref, sems, 0)
    run(copies + router_copies(f, chip(f, 0, 4 - dx), piece_ref.at[pl.ds(count, 4)], router_ref, sems, 2))


def place_relayed(dx, f, piece, final, router):
    return pl.pallas_call(
        functools.partial(place_relayed_kernel, dx),
        out_shape=[array(*final.shape), array(*router.shape)],
        in_specs=[SMEM, VMEM, ANY, ANY],
        out_specs=[ANY, ANY],
        scratch_shapes=[pltpu.SemaphoreType.DMA((6,))],
        input_output_aliases={2: 0, 3: 1},
        compiler_params=params(2),
        cost_estimate=cost(2**18, 2**18),
        name="place_relayed",
    )(f, piece, final, router)


def served(w, router_weight, router_gain):
    experts, _, _ = w.shape
    direct = experts - RELAY - EARLY
    position = lax.axis_index("fsdp")
    f = position.reshape(1)
    y = lax.axis_index("ep").reshape(1)
    far_plane, core = 1 - position // 8, position % 2

    scale, scale_theirs, swap, swap_rest = local_maxima(f, w)
    scale = jnp.maximum(scale, send(scale_theirs, 0, 0, 1))
    peer = send(scale, 1, 0, 0)
    product = router_weight.T * router_gain.reshape(1, -1)
    early = lax.dynamic_slice(w, (experts - EARLY, 512 * far_plane, 0), (EARLY, 512, 128))
    early = jnp.concatenate([early.reshape(-1, 128), product])
    early = send(early, 1, 0, 0)
    theirs = send(swap, 0, 0, 1)
    scale = jnp.maximum(scale, peer)
    scale = functools.reduce(jnp.maximum, [scale] + [send(scale, 0, dx, 0) for dx in (1, 3, 2)])
    rest = send(swap_rest, 0, 0, 1)

    (chunk,) = far_pieces(f, w, theirs, scale, 0, RELAY, True)
    forward = send(chunk, 1, 0, 0)
    turned = early[: 512 * EARLY].reshape(EARLY, 4, 2, 64, 128)
    turned = lax.dynamic_slice_in_dim(turned, 1 - core, 1, axis=2).reshape(EARLY * 256, 128)
    turned = send(turned, 0, 0, 1)
    *pieces, final = near_pieces(f, w, scale, early, turned, theirs, rest)
    plane = [send(piece, 0, k + 1, 0) for k, piece in enumerate(pieces)]
    pieces = far_pieces(f, w, rest, scale, RELAY, direct, False)
    across = [send(piece, 1, k, 0) for k, piece in enumerate(pieces)]
    near = jnp.stack([product, early[-16:]]).astype(BF16)
    near = jnp.concatenate([near, send(near, 0, 0, 1)])
    received = [near]
    for d in (1, 2, 3):
        received.append(lax.ppermute(near, "ep", [(i, (i + d) % 4) for i in range(4)]))
    *pieces, final, router = split(f, y, forward, received, final)
    relayed = [send(piece, 0, k + 1, 0) for k, piece in enumerate(pieces)]
    for k in range(3):
        final = place_near(k + 1, f, plane[k], final)
    for k in range(3):
        final, router = place_relayed(k + 1, f, relayed[k], final, router)
    for k in range(4):
        final = place_far(k, RELAY, f, across[k], final)
    own = lax.dynamic_slice_in_dim(scale, position // 2 * 64, 64, axis=1)
    return final, own, router.T


def solution(mesh):
    return jax.shard_map(
        served,
        mesh=mesh,
        in_specs=(
            P(("trial", "ep"), None, "fsdp"),
            P(("trial", "fsdp"), "ep"),
            P(("trial", "fsdp")),
        ),
        out_specs=(P(("trial", "ep"), "fsdp", None), P(("trial", "ep"), "fsdp"), P("trial", None)),
        check_vma=False,
    )
```
